32 devices in a mesh: rows: 8 (over y, x, core), model: 4 (over z).
Axes of the slice: x: 2, y: 2, z: 4, core: 2. Of those that a mesh axis runs over, the one named last changes fastest.
Arguments:
- weight_gate: bfloat16 [2048, 8192], P('rows', 'model'), may hold values from -0.125 to 0.125
- low_gate: bfloat16 [2048, 64], P('rows'), may hold values from -0.125 to 0.125
- high_gate: bfloat16 [64, 8192], P(None, 'model'), may hold values from -0.75 to 0.75
- weight_up: bfloat16 [2048, 8192], P('rows', 'model'), may hold values from -0.125 to 0.125
- low_up: bfloat16 [2048, 64], P('rows'), may hold values from -0.125 to 0.125
- high_up: bfloat16 [64, 8192], P(None, 'model'), may hold values from -0.75 to 0.75
- weight_down: bfloat16 [8192, 2048], P('model', 'rows'), may hold values from -0.0625 to 0.0625
- low_down: bfloat16 [8192, 64], P('model'), may hold values from -0.0625 to 0.0625
- high_down: bfloat16 [64, 2048], P(None, 'rows'), may hold values from -0.75 to 0.75
- norm_train: float32 [2048], P(('rows', 'model')), may hold values from 0.25 to 1.75
- norm_step: float32 [2048], P(('rows', 'model')), may hold values from -0.3 to 0.3
Outputs:
- final_gate: bfloat16 [8192, 2048], P('model')
- final_up: bfloat16 [8192, 2048], P('model')
- final_down: bfloat16 [2048, 8192], P(None, 'model')
- serve_norm: bfloat16 [2048], replicated
The draws below stay inside these ranges and needn't reach their ends.
All inputs are finite; a program needn't handle non-finite values.
Results may differ from the reference program's by a relative error of at most 0.001.
Values may be sent and summed in bfloat16 or wider, within the bound.
A program may use at most 192 MiB of HBM per device.

```python
import jax
import jax.numpy as jnp

D_MODEL = 2048
D_INNER = 8192
RANK = 64


def block_scale(own_key, extent, split, least, top_value):
    def one(position, shards_of):
        steps = jax.random.uniform(jax.random.fold_in(jax.random.fold_in(own_key, 6), position), (shards_of,), jnp.float32, least / len(split), top_value / len(split))
        return jnp.repeat(jnp.exp(steps), extent[position] // shards_of).reshape((-1,) + (1,) * (len(extent) - position - 1))

    level = one(*split[0])
    for cut in split[1:]:
        level = level * one(*cut)
    return level


def bell_draw(rng, shape, scale, limit, pieces=(), dtype=jnp.bfloat16):
    drawn = jax.random.normal(rng, shape, jnp.float32) * scale
    if len(pieces) > 0:
        drawn = block_scale(rng, shape, pieces, -0.22, 0.18) * drawn
    return jnp.clip(drawn, min=-limit, max=limit).astype(dtype)


def setup_inputs(seed: int = 0) -> dict:
    keys = jax.random.split(jax.random.key(seed), 12)
    return {
        "weight_gate": bell_draw(keys[0], (D_MODEL, D_INNER), D_MODEL ** -0.5, 0.125, ((0, 8), (1, 4))),
        "low_gate": bell_draw(keys[1], (D_MODEL, RANK), D_MODEL ** -0.5, 0.125, ((0, 8),)),
        "high_gate": bell_draw(keys[2], (RANK, D_INNER), RANK ** -0.5, 0.75, ((1, 4),)),
        "weight_up": bell_draw(keys[3], (D_MODEL, D_INNER), D_MODEL ** -0.5, 0.125, ((0, 8), (1, 4))),
        "low_up": bell_draw(keys[4], (D_MODEL, RANK), D_MODEL ** -0.5, 0.125, ((0, 8),)),
        "high_up": bell_draw(keys[5], (RANK, D_INNER), RANK ** -0.5, 0.75, ((1, 4),)),
        "weight_down": bell_draw(keys[6], (D_INNER, D_MODEL), D_INNER ** -0.5, 0.0625, ((0, 4), (1, 8))),
        "low_down": bell_draw(keys[7], (D_INNER, RANK), D_INNER ** -0.5, 0.0625, ((0, 4),)),
        "high_down": bell_draw(keys[8], (RANK, D_MODEL), RANK ** -0.5, 0.75, ((1, 8),)),
        "norm_train": jnp.clip(1.0 + 0.15 * jax.random.normal(keys[9], (D_MODEL,), jnp.float32), 0.25, 1.75),
        "norm_step": jnp.clip(jax.random.uniform(keys[10], (D_MODEL,), jnp.float32, -0.3, 0.3) * block_scale(keys[10], (D_MODEL,), ((0, 32),), -0.4, 0.0), -0.3, 0.3),
    }


mix_rate = 0.5


def reference(weight_gate, low_gate, high_gate, weight_up, low_up, high_up, weight_down, low_down, high_down, norm_train, norm_step):
    result_gate = weight_gate.astype(jnp.float32) + mix_rate * jnp.dot(low_gate, high_gate, preferred_element_type=jnp.float32)
    result_up = weight_up.astype(jnp.float32) + mix_rate * jnp.dot(low_up, high_up, preferred_element_type=jnp.float32)
    result_down = weight_down.astype(jnp.float32) + mix_rate * jnp.dot(low_down, high_down, preferred_element_type=jnp.float32)
    final_gate = result_gate.T.astype(jnp.bfloat16)
    final_up = result_up.T.astype(jnp.bfloat16)
    final_down = result_down.T.astype(jnp.bfloat16)
    serve_norm = (norm_train + norm_step).astype(jnp.bfloat16)
    return final_gate, final_up, final_down, serve_norm
```

```python
import functools

import jax
import jax.numpy as jnp
from jax import lax
from jax.experimental import pallas as pl
from jax.experimental.pallas import tpu as pltpu
from jax.sharding import PartitionSpec as P

mix_rate = 0.5
MESH = pl.DeviceIdType.MESH
PIECES = 4
STRIPS = 1
DOWN_PIECES = 8
EARLY = 6
SIDE = 2


class Place:
    def __init__(self):
        self.me = me = lax.axis_index("rows")
        self.core = core = lax.rem(me, 2)
        x = lax.rem(me // 2, SIDE)
        y = me // (2 * SIDE)

        def device(y, x, core):
            return (y * SIDE + x) * 2 + core

        self.near_x, self.near_y = device(y, 1 - x, core), device(1 - y, x, core)
        self.far = device(1 - y, 1 - x, core)
        self.pair = device(y, x, 1 - core)
        self.pair_x, self.pair_y = device(y, 1 - x, 1 - core), device(1 - y, x, 1 - core)
        self.pair_far = device(1 - y, 1 - x, 1 - core)


def remote(src, dst, send, recv, target):
    return pltpu.make_async_remote_copy(
        src_ref=src, dst_ref=dst, send_sem=send, recv_sem=recv, device_id={"rows": target}, device_id_type=MESH
    )


def shifted(position, size, step):
    return lax.rem(position + step, size)


def first_kernel(rows, model, *refs):
    sources, (og, ou, own, early, norm), refs = refs[:11], refs[11:16], refs[16:]
    held, refs = refs[:11], refs[11:]
    wg, lg, hg, wu, lu, hu, wd, ld, hd, nt, ns = held
    fetch_sem, link_send, link_recv, pair_send, pair_recv, early_send, early_recv, norm_send, norm_recv = refs
    at = Place()
    me, near_x, near_y, far, pair = at.me, at.near_x, at.near_y, at.far, at.pair
    depth = lax.axis_index("model")

    barrier = pltpu.get_barrier_semaphore()
    for step in range(1, rows):
        pl.semaphore_signal(barrier, inc=1, device_id={"rows": shifted(me, rows, step)}, device_id_type=MESH)
    for step in range(1, model):
        pl.semaphore_signal(barrier, inc=1, device_id={"model": shifted(depth, model, step)}, device_id_type=MESH)

    outs = (og, ou)
    fetches = {}

    def fetch(key, i, *cut):
        fetches[key] = pltpu.make_async_copy(
            sources[i].at[cut] if cut else sources[i], held[i].at[cut] if cut else held[i],
            fetch_sem.at[len(fetches)],
        )

    long = wg.shape[1] // PIECES
    long_down = wd.shape[0] // PIECES
    short = wg.shape[0]
    short_down = wd.shape[1]
    units = [(a, k) for k in range(PIECES) for a in range(2)]
    count = len(units)
    work = units + [(2, k) for k in range(PIECES)]

    for u, (a, k) in enumerate(work):
        if k == 0:
            fetch(("low", a), 3 * a + 1)
            fetch(("high", a), 3 * a + 2)
        if a < 2:
            fetch(u, 3 * a, pl.ds(0, short), pl.ds(k * long, long))
        else:
            fetch(u, 3 * a, pl.ds(k * long_down, long_down), pl.ds(0, short_down))
    fetch("train", 9)
    fetch("step", 10)
    for f in fetches.values():
        f.start()

    def place(u, owner):
        a, k = units[u]
        return outs[a].at[pl.ds(k * long, long), pl.ds(pl.multiple_of(owner * short, short), short)]

    def compute(u):
        a, k = work[u]
        if k == 0:
            fetches["low", a].wait()
            fetches["high", a].wait()
        fetches[u].wait()
        if a < 2:
            w, low, high = ((wg, lg, hg), (wu, lu, hu))[a]
            cut = slice(k * long, (k + 1) * long)
            weight, low, high = w[:, cut], low[...], high[:, cut]
        else:
            cut = slice(k * long_down, (k + 1) * long_down)
            weight, low, high = wd[cut, :], ld[:, cut], hd[...]
        merged = weight.astype(jnp.float32) + mix_rate * lax.dot_general(
            low, high, (((0,), (0,)), ((), ())), preferred_element_type=jnp.float32
        )
        merged = merged.astype(jnp.bfloat16).T
        if a < 2:
            place(u, me)[...] = merged
        else:
            own[:, cut] = merged

    def copy(u, owner, send, recv, target):
        return remote(place(u, owner), place(u, owner), send, recv, target)

    def link(lane, u, owner, target):
        return copy(u, owner, link_send.at[lane, u], link_recv.at[lane, u], target)

    def across(lane, u, owner):
        return copy(u, owner, pair_send.at[lane, u], pair_recv.at[lane, u], pair)

    piece = own.shape[1] // DOWN_PIECES

    def ahead(lane, k, src, target):
        cut = (slice(None), pl.ds(k * piece, piece))
        src = own.at[cut] if src is None else early.at[(src, *cut)]
        return remote(src, early.at[(lane, *cut)], early_send.at[lane, k], early_recv.at[lane, k], target)

    def send_own(u):
        link(0, u, me, near_x).start()
        link(1, u, me, near_y).start()
        across(3, u, me).start()

    compute(0)
    fetches["train"].wait()
    fetches["step"].wait()
    norm[me, depth] = jnp.zeros(norm.shape[2:], norm.dtype)
    norm[me, depth, :, : nt.shape[1]] = nt[...] + ns[...]
    pl.semaphore_wait(barrier, rows - 1 + model - 1)
    for u in range(1, count):
        compute(u)
        send_own(u - 1)
    compute(count)
    send_own(count - 1)
    for u in range(count + 1, len(work)):
        compute(u)

    def norm_copy(step, send):
        if step < model:
            to = {"model": shifted(depth, model, step)}
            ref = norm.at[me, depth] if send else norm.at[me, shifted(depth, model, model - step)]
            slot = step - 1
        else:
            step = step - model + 1
            to = {"rows": shifted(me, rows, step)}
            ref = norm.at[me] if send else norm.at[shifted(me, rows, rows - step)]
            slot = model - 1 + step - 1
        return pltpu.make_async_remote_copy(
            src_ref=ref, dst_ref=ref, send_sem=norm_send.at[slot], recv_sem=norm_recv.at[slot],
            device_id=to, device_id_type=MESH,
        )

    for step in range(1, model):
        norm_copy(step, True).start()
    for step in range(1, model):
        norm_copy(step, False).wait_recv()
    for step in range(model, model + rows - 1):
        norm_copy(step, True).start()

    for u in range(count):
        link(0, u, near_x, near_x).wait_recv()
        if u % 2 == 0:
            link(2, u, near_x, near_y).start()
        across(0, u, near_x).start()
        link(1, u, near_y, near_y).wait_recv()
        if u % 2 == 1:
            link(2, u, near_y, near_x).start()
        across(1, u, near_y).start()

    @pl.when(at.core == 1)
    def _():
        for k in range(EARLY):
            ahead(0, k, None, near_x).start()
            ahead(1, k, None, near_y).start()

    for u in range(count):
        link(2, u, far, near_x).wait_recv()
        across(2, u, far).start()

    @pl.when(at.core == 1)
    def _():
        for k in range(EARLY):
            ahead(0, k, None, near_x).wait_recv()
            if k % 2 == 0:
                ahead(2, k, 0, near_y).start()
            ahead(1, k, None, near_y).wait_recv()
            if k % 2 == 1:
                ahead(2, k, 1, near_x).start()

    for step in range(model, model + rows - 1):
        norm_copy(step, False).wait_recv()
    for step in range(1, model + rows - 1):
        norm_copy(step, True).wait_send()
    for u in range(count):
        link(0, u, me, near_x).wait_send()
        link(1, u, me, near_y).wait_send()
        link(2, u, near_x if u % 2 == 0 else near_y, near_x).wait_send()
        for lane, mine, theirs in ((3, me, pair), (0, near_x, at.pair_x), (1, near_y, at.pair_y), (2, far, at.pair_far)):
            across(lane, u, mine).wait_send()
            across(lane, u, theirs).wait_recv()

    @pl.when(at.core == 1)
    def _():
        for k in range(EARLY):
            ahead(0, k, None, near_x).wait_send()
            ahead(1, k, None, near_y).wait_send()
            ahead(2, k, k % 2, near_x).wait_send()
            ahead(2, k, None, near_x).wait_recv()


def second_kernel(own, early, token, down, link_send, link_recv, pair_send, pair_recv, ready):
    at = Place()
    me, near_x, near_y, far, pair = at.me, at.near_x, at.near_y, at.far, at.pair
    short = own.shape[0]
    piece = own.shape[1] // DOWN_PIECES

    barrier = pltpu.get_barrier_semaphore()
    for near in (near_x, near_y):
        pl.semaphore_signal(barrier, inc=1, device_id={"rows": near}, device_id_type=MESH)
    pl.semaphore_wait(barrier, 2 + at.core)

    def cut(k):
        return slice(None), pl.ds(k * piece, piece)

    def band(owner):
        return pl.ds(pl.multiple_of(owner * short, short), short)

    def place(k, owner):
        return down.at[band(owner), pl.ds(k * piece, piece)]

    def link(lane, k, src, owner, target):
        return remote(src, place(k, owner), link_send.at[lane, k], link_recv.at[lane, k], target)

    def across(lane, k, src, owner):
        return remote(src, place(k, owner), pair_send.at[lane, k], pair_recv.at[lane, k], pair)

    def gather(first, meet):
        pieces, everything = range(first, DOWN_PIECES), range(DOWN_PIECES)
        for k in pieces:
            link(0, k, own.at[cut(k)], me, near_x).start()
            link(1, k, own.at[cut(k)], me, near_y).start()
        down[band(me), :] = own[...]

        def over():
            for k in everything:
                across(3, k, own.at[cut(k)], me).start()
            for k in range(first):
                for lane, owner in enumerate((near_x, near_y, far)):
                    across(lane, k, early.at[(lane, *cut(k))], owner).start()
            for lane, owner in enumerate((near_x, near_y, far)):
                if first:
                    down[band(owner), : first * piece] = early[lane]

        if first:
            over()
        for k in pieces:
            link(0, k, place(k, near_x), near_x, near_x).wait_recv()
            if k % 2 == 0:
                link(2, k, place(k, near_x), near_x, near_y).start()
            link(1, k, place(k, near_y), near_y, near_y).wait_recv()
            if k % 2 == 1:
                link(2, k, place(k, near_y), near_y, near_x).start()
        if not first:
            pl.semaphore_wait(ready, 1)
            over()
        for k in pieces:
            across(0, k, place(k, near_x), near_x).start()
            across(1, k, place(k, near_y), near_y).start()
        for k in pieces:
            link(2, k, place(k, far), far, near_x).wait_recv()
            across(2, k, place(k, far), far).start()

        for k in pieces:
            link(0, k, own.at[cut(k)], me, near_x).wait_send()
            link(1, k, own.at[cut(k)], me, near_y).wait_send()
            link(2, k, place(k, near_x), near_x, near_x).wait_send()
        for k in everything:
            for lane, mine, theirs in ((3, me, pair), (0, near_x, at.pair_x), (1, near_y, at.pair_y), (2, far, at.pair_far)):
                across(lane, k, place(k, mine), mine).wait_send()
                across(lane, k, place(k, theirs), theirs).wait_recv()

    @pl.when(at.core == 0)
    def _():
        pl.semaphore_signal(barrier, inc=1, device_id={"rows": pair}, device_id_type=MESH)
        gather(0, True)

    @pl.when(at.core == 1)
    def _():
        pl.semaphore_signal(ready, inc=1, device_id={"rows": pair}, device_id_type=MESH)
        gather(EARLY, False)


HBM = pl.BlockSpec(memory_space=pltpu.HBM)
VMEM = pl.BlockSpec(memory_space=pltpu.VMEM)
MIB = 2**20


def first_gather(rows, model, arrays):
    weight_gate, weight_up, weight_down, norm_train = arrays[0], arrays[3], arrays[6], arrays[9]
    own = (weight_down.shape[1], weight_down.shape[0])
    shapes = [
        (weight_gate.shape[1], weight_gate.shape[0] * rows),
        (weight_up.shape[1], weight_up.shape[0] * rows),
        own,
        (3, own[0], own[1] // DOWN_PIECES * EARLY),
    ]
    lanes = -(-norm_train.shape[1] // 128) * 128
    count = 2 * PIECES
    small = rows - 1 + model - 1
    dma = pltpu.SemaphoreType.DMA
    return pl.pallas_call(
        functools.partial(first_kernel, rows, model),
        out_shape=[pltpu.VMEM(s, jnp.bfloat16) for s in shapes] + [pltpu.VMEM((rows, model, 1, lanes), jnp.float32)],
        in_specs=[HBM] * len(arrays),
        out_specs=[VMEM] * 5,
        scratch_shapes=[pltpu.VMEM(a.shape, a.dtype) for a in arrays]
        + [
            dma((3 * PIECES + 8,)),
            dma((3, count)), dma((3, count)), dma((4, count)), dma((4, count)),
            dma((3, EARLY)), dma((3, EARLY)), dma((small,)), dma((small,)),
        ],
        compiler_params=pltpu.CompilerParams(collective_id=0, has_side_effects=True, vmem_limit_bytes=44 * MIB + MIB // 4),
    )(*arrays)


def second_gather(rows, own, early, token):
    dma = pltpu.SemaphoreType.DMA
    return pl.pallas_call(
        second_kernel,
        out_shape=pltpu.VMEM((own.shape[0] * rows, own.shape[1]), jnp.bfloat16),
        in_specs=[VMEM, VMEM, HBM],
        out_specs=VMEM,
        scratch_shapes=[
            dma((3, DOWN_PIECES)), dma((3, DOWN_PIECES)), dma((4, DOWN_PIECES)), dma((4, DOWN_PIECES)),
            pltpu.SemaphoreType.REGULAR,
        ],
        compiler_params=pltpu.CompilerParams(collective_id=1, has_side_effects=True, vmem_limit_bytes=4 * MIB),
    )(own, early, token)


def write_kernel(size, lanes, g, u, norm, og, ou, out, token, sems):
    copies = [pltpu.make_async_copy(s, t, sems.at[i]) for i, (s, t) in enumerate(((g, og), (u, ou)))]
    for c in copies:
        c.start()
    rows, model = norm.shape[:2]
    parts = [norm[r, m][:, :size] for r in range(rows) for m in range(model)]
    group = lanes // size
    packed = [jnp.concatenate(parts[i : i + group], axis=1) for i in range(0, len(parts), group)]
    out[...] = jnp.concatenate(packed, axis=0).astype(out.dtype)
    token[...] = jnp.zeros(token.shape, token.dtype)
    for c in copies:
        c.wait()


def written(size, arrays):
    lanes = arrays[2].shape[3]
    total = arrays[2].shape[0] * arrays[2].shape[1] * size
    return pl.pallas_call(
        functools.partial(write_kernel, size, lanes),
        out_shape=[jax.ShapeDtypeStruct(a.shape, a.dtype) for a in arrays[:2]]
        + [jax.ShapeDtypeStruct((total // lanes, lanes), jnp.bfloat16), jax.ShapeDtypeStruct((8, 128), jnp.float32)],
        in_specs=[VMEM] * 3,
        out_specs=[HBM] * 2 + [VMEM] * 2,
        scratch_shapes=[pltpu.SemaphoreType.DMA((2,))],
        compiler_params=pltpu.CompilerParams(vmem_limit_bytes=MIB),
    )(*arrays)


def last_kernel(d, od, sem):
    c = pltpu.make_async_copy(d, od, sem)
    c.start()
    c.wait()


def last_written(down):
    return pl.pallas_call(
        last_kernel,
        out_shape=jax.ShapeDtypeStruct(down.shape, down.dtype),
        in_specs=[VMEM],
        out_specs=HBM,
        scratch_shapes=[pltpu.SemaphoreType.DMA(())],
        compiler_params=pltpu.CompilerParams(vmem_limit_bytes=MIB),
    )(down)


def local_kernel(rows, model, *arrays):
    arrays = tuple(a.T if i in (1, 4, 7) else a for i, a in enumerate(arrays[:9])) + tuple(
        a.reshape(1, -1) for a in arrays[9:]
    )
    gate, up, own, early, norm = first_gather(rows, model, arrays)
    gate, up, serve_norm, token = written(arrays[9].shape[1], (gate, up, norm))
    down = last_written(second_gather(rows, own, early, token))
    return gate, up, down, serve_norm.reshape(-1)


def merge(weight, low, high):
    full = weight.astype(jnp.float32) + mix_rate * jnp.dot(low, high, preferred_element_type=jnp.float32)
    return full.astype(jnp.bfloat16).T


def local_plain(*arrays):
    gate, up, down = merge(*arrays[:3]), merge(*arrays[3:6]), merge(*arrays[6:9])
    return (
        lax.all_gather(gate, "rows", axis=1, tiled=True),
        lax.all_gather(up, "rows", axis=1, tiled=True),
        lax.all_gather(down, "rows", axis=0, tiled=True),
        lax.all_gather((arrays[9] + arrays[10]).astype(jnp.bfloat16), ("rows", "model"), axis=0, tiled=True),
    )


def solution(mesh):
    rows, model = mesh.shape["rows"], mesh.shape["model"]
    local = functools.partial(local_kernel, rows, model) if rows == 2 * SIDE * SIDE else local_plain
    in_specs = (
        P("rows", "model"), P("rows", None), P(None, "model"),
        P("rows", "model"), P("rows", None), P(None, "model"),
        P("model", "rows"), P("model", None), P(None, "rows"),
        P(("rows", "model")), P(("rows", "model")),
    )
    out_specs = (P("model", None), P("model", None), P(None, "model"), P())
    return jax.shard_map(local, mesh=mesh, in_specs=in_specs, out_specs=out_specs, check_vma=False)
```

```python
import functools

import jax
import jax.numpy as jnp
from jax import lax
from jax.experimental import pallas as pl
from jax.experimental.pallas import tpu as pltpu
from jax.sharding import PartitionSpec as P

mix_rate = 0.5
MESH = pl.DeviceIdType.MESH
UNITS = ((1, 1, 3, 3, 4, 4), (4, 4, 3, 3, 1, 1))
DOWN = (2, 2, 2, 2, 2, 2, 1, 1, 1, 1)
EARLY = 8
SIDE = 2


def cuts(parts, size):
    whole = sum(parts)
    return [(sum(parts[:i]) * size // whole, parts[i] * size // whole) for i in range(len(parts))]


class Place:
    def __init__(self):
        self.me = me = lax.axis_index("rows")
        self.core = core = lax.rem(me, 2)
        x = lax.rem(me // 2, SIDE)
        y = me // (2 * SIDE)

        def device(y, x, core):
            return (y * SIDE + x) * 2 + core

        self.near_x, self.near_y = device(y, 1 - x, core), device(1 - y, x, core)
        self.far = device(1 - y, 1 - x, core)
        self.pair = device(y, x, 1 - core)
        self.pair_x, self.pair_y = device(y, 1 - x, 1 - core), device(1 - y, x, 1 - core)
        self.pair_far = device(1 - y, 1 - x, 1 - core)


def remote(src, dst, send, recv, target):
    return pltpu.make_async_remote_copy(
        src_ref=src, dst_ref=dst, send_sem=send, recv_sem=recv,
        device_id=target if isinstance(target, dict) else {"rows": target}, device_id_type=MESH,
    )


def first_kernel(*refs):
    sources, (og, ou, own, early, norm), refs = refs[:11], refs[11:16], refs[16:]
    held, refs = refs[:11], refs[11:]
    wg, lg, hg, wu, lu, hu, wd, ld, hd, nt, ns = held
    fetch_sem, link_send, link_recv, pair_send, pair_recv, early_send, early_recv = refs
    at = Place()
    me, near_x, near_y, far, pair = at.me, at.near_x, at.near_y, at.far, at.pair

    barrier = pltpu.get_barrier_semaphore()
    for other in (near_x, near_y, pair):
        pl.semaphore_signal(barrier, inc=1, device_id={"rows": other}, device_id_type=MESH)

    outs = (og, ou)
    fetches = {}

    def fetch(key, i, *cut):
        fetches[key] = pltpu.make_async_copy(
            sources[i].at[cut] if cut else sources[i], held[i].at[cut] if cut else held[i],
            fetch_sem.at[len(fetches)],
        )

    short, short_down = wg.shape[0], wd.shape[1]
    units = [(a, *cut) for a in range(2) for cut in cuts(UNITS[a], wg.shape[1])]
    count = len(units)
    work = units + [(2, *cut) for cut in cuts((1, 1, 1, 1), wd.shape[0])]
    whole = slice(None)

    for u, (a, start, size) in enumerate(work):
        if start == 0:
            fetch(("low", a), 3 * a + 1)
            if a < 2:
                fetch(("high", a), 3 * a + 2, whole, pl.ds(0, size))
            else:
                fetch(("high", a), 3 * a + 2)
        if a < 2:
            fetch(u, 3 * a, whole, pl.ds(start, size))
        else:
            fetch(u, 3 * a, pl.ds(start, size), whole)
        if start == 0 and a < 2:
            fetch(("rest", a), 3 * a + 2, whole, pl.ds(size, wg.shape[1] - size))
    fetch("train", 9)
    fetch("step", 10)
    for f in fetches.values():
        f.start()

    def place(u, owner):
        a, start, size = units[u]
        return outs[a].at[pl.ds(start, size), pl.ds(pl.multiple_of(owner * short, short), short)]

    def compute(u):
        a, start, size = work[u]
        if start == 0:
            fetches["low", a].wait()
            fetches["high", a].wait()
        elif a < 2 and work[u - 1][1] == 0:
            fetches["rest", a].wait()
        fetches[u].wait()
        cut = slice(start, start + size)
        if a < 2:
            w, low, high = ((wg, lg, hg), (wu, lu, hu))[a]
            weight, low, high = w[:, cut], low[...], high[:, cut]
        else:
            weight, low, high = wd[cut, :], ld[:, cut], hd[...]
        merged = weight.astype(jnp.float32) + mix_rate * lax.dot_general(
            low, high, (((0,), (0,)), ((), ())), preferred_element_type=jnp.float32
        )
        merged = merged.astype(jnp.bfloat16).T
        if a < 2:
            place(u, me)[...] = merged
        else:
            own[:, cut] = merged

    def copy(u, owner, send, recv, target):
        return remote(place(u, owner), place(u, owner), send, recv, target)

    def link(lane, u, owner, target):
        return copy(u, owner, link_send.at[lane, u], link_recv.at[lane, u], target)

    def across(lane, u, owner):
        return copy(u, owner, pair_send.at[lane, u], pair_recv.at[lane, u], pair)

    pieces = cuts(DOWN, own.shape[1])[:EARLY]

    def ahead(lane, k, src, target):
        cut = (whole, pl.ds(*pieces[k]))
        src = own.at[cut] if src is None else early.at[(src, *cut)]
        return remote(src, early.at[(lane, *cut)], early_send.at[lane, k], early_recv.at[lane, k], target)

    def send_own(u):
        link(0, u, me, near_x).start()
        link(1, u, me, near_y).start()
        across(3, u, me).start()

    compute(0)
    pl.semaphore_wait(barrier, 3)
    for u in range(1, count + 1):
        compute(u)
        send_own(u - 1)
    for u in range(count + 1, len(work)):
        compute(u)
    fetches["train"].wait()
    fetches["step"].wait()
    norm[...] = jnp.zeros(norm.shape, norm.dtype)
    norm[:, : nt.shape[1]] = nt[...] + ns[...]

    for u in range(count):
        link(0, u, near_x, near_x).wait_recv()
        if u % 2 == 0:
            link(2, u, near_x, near_y).start()
        across(0, u, near_x).start()
        link(1, u, near_y, near_y).wait_recv()
        if u % 2 == 1:
            link(2, u, near_y, near_x).start()
        across(1, u, near_y).start()

    @pl.when(at.core == 1)
    def _():
        for k in range(EARLY):
            ahead(0, k, None, near_x).start()
            ahead(1, k, None, near_y).start()

    for u in range(count):
        link(2, u, far, near_x).wait_recv()
        across(2, u, far).start()

    @pl.when(at.core == 1)
    def _():
        for k in range(EARLY):
            ahead(0, k, None, near_x).wait_recv()
            if k % 2 == 0:
                ahead(2, k, 0, near_y).start()
            ahead(1, k, None, near_y).wait_recv()
            if k % 2 == 1:
                ahead(2, k, 1, near_x).start()

    for u in range(count):
        link(0, u, me, near_x).wait_send()
        link(1, u, me, near_y).wait_send()
        link(2, u, near_x, near_x).wait_send()
        for lane, mine, theirs in ((3, me, pair), (0, near_x, at.pair_x), (1, near_y, at.pair_y), (2, far, at.pair_far)):
            across(lane, u, mine).wait_send()
            across(lane, u, theirs).wait_recv()

    @pl.when(at.core == 1)
    def _():
        for k in range(EARLY):
            ahead(0, k, None, near_x).wait_send()
            ahead(1, k, None, near_y).wait_send()
            ahead(2, k, k % 2, near_x).wait_send()
            ahead(2, k, None, near_x).wait_recv()


def second_kernel(model, own, early, part, token, down, norm, *sems):
    link_send, link_recv, pair_send, pair_recv, norm_send, norm_recv, ready = sems
    at = Place()
    me, near_x, near_y, far, pair = at.me, at.near_x, at.near_y, at.far, at.pair
    depth = lax.axis_index("model")
    short = own.shape[0]
    pieces = cuts(DOWN, own.shape[1])

    barrier = pltpu.get_barrier_semaphore()
    for other in (near_x, near_y, far):
        pl.semaphore_signal(barrier, inc=1, device_id={"rows": other}, device_id_type=MESH)
    for step in range(1, model):
        pl.semaphore_signal(barrier, inc=1, device_id={"model": lax.rem(depth + step, model)}, device_id_type=MESH)
    norm[me, depth] = part[...]
    pl.semaphore_wait(barrier, 2 + model + at.core)

    def cut(k):
        return slice(None), pl.ds(*pieces[k])

    def band(owner):
        return pl.ds(pl.multiple_of(owner * short, short), short)

    def place(k, owner):
        return down.at[band(owner), pl.ds(*pieces[k])]

    def link(lane, k, src, owner, target):
        return remote(src, place(k, owner), link_send.at[lane, k], link_recv.at[lane, k], target)

    def across(lane, k, src, owner):
        return remote(src, place(k, owner), pair_send.at[lane, k], pair_recv.at[lane, k], pair)

    def norm_copy(slot, ref, target):
        return remote(ref, ref, norm_send.at[slot], norm_recv.at[slot], target)

    rings = range(1, model)
    rows_mine = ((me, pair), (near_x, at.pair_x), (near_y, at.pair_y), (far, at.pair_far))

    def norm_deep(step):
        return norm_copy(step - 1, norm.at[me, depth], {"model": lax.rem(depth + step, model)})

    def norm_deep_back(step):
        return norm_copy(step - 1, norm.at[me, lax.rem(depth + model - step, model)], {"model": lax.rem(depth + step, model)})

    def norm_wide(lane, owner, target):
        return norm_copy(model - 1 + lane, norm.at[owner], target)

    def norm_across(lane, owner):
        return norm_copy(model + 2 + lane, norm.at[owner], pair)

    def gather(first):
        late, everything = range(first, len(pieces)), range(len(pieces))
        for k in late:
            link(0, k, own.at[cut(k)], me, near_x).start()
            link(1, k, own.at[cut(k)], me, near_y).start()
        for step in rings:
            norm_deep(step).start()

        def over():
            for k in everything:
                across(3, k, own.at[cut(k)], me).start()
            for k in range(first):
                for lane, owner in enumerate((near_x, near_y, far)):
                    across(lane, k, early.at[(lane, *cut(k))], owner).start()

        def spread():
            for step in rings:
                norm_deep_back(step).wait_recv()
            for lane, owner in enumerate((near_x, near_y, far)):
                norm_wide(lane, me, owner).start()

        if first:
            over()
        down[band(me), :] = own[...]
        if first:
            end = sum(pieces[first - 1])
            for lane, owner in enumerate((near_x, near_y, far)):
                down[band(owner), :end] = early[lane]
        for k in late:
            link(0, k, place(k, near_x), near_x, near_x).wait_recv()
            if k % 2 == 0:
                link(2, k, place(k, near_x), near_x, near_y).start()
            link(1, k, place(k, near_y), near_y, near_y).wait_recv()
            if k % 2 == 1:
                link(2, k, place(k, near_y), near_y, near_x).start()
            if k == first + 1:
                spread()
        if not first:
            pl.semaphore_wait(ready, 1)
            over()
        for k in late:
            across(0, k, place(k, near_x), near_x).start()
            across(1, k, place(k, near_y), near_y).start()
        for lane, owner in enumerate((near_x, near_y, far)):
            norm_wide(lane, owner, owner).wait_recv()
        for lane, (mine, _) in enumerate(rows_mine):
            norm_across(lane, mine).start()
        for k in late:
            link(2, k, place(k, far), far, near_x).wait_recv()
            across(2, k, place(k, far), far).start()

        for step in rings:
            norm_deep(step).wait_send()
        for lane, owner in enumerate((near_x, near_y, far)):
            norm_wide(lane, me, owner).wait_send()
        for lane, (mine, theirs) in enumerate(rows_mine):
            norm_across(lane, mine).wait_send()
            norm_across(lane, theirs).wait_recv()
        for k in late:
            link(0, k, own.at[cut(k)], me, near_x).wait_send()
            link(1, k, own.at[cut(k)], me, near_y).wait_send()
            link(2, k, place(k, near_x), near_x, near_x).wait_send()
        for k in everything:
            for lane, mine, theirs in ((3, me, pair), (0, near_x, at.pair_x), (1, near_y, at.pair_y), (2, far, at.pair_far)):
                across(lane, k, place(k, mine), mine).wait_send()
                across(lane, k, place(k, theirs), theirs).wait_recv()

    @pl.when(at.core == 0)
    def _():
        pl.semaphore_signal(barrier, inc=1, device_id={"rows": pair}, device_id_type=MESH)
        gather(0)

    @pl.when(at.core == 1)
    def _():
        pl.semaphore_signal(ready, inc=1, device_id={"rows": pair}, device_id_type=MESH)
        gather(EARLY)


HBM = pl.BlockSpec(memory_space=pltpu.HBM)
VMEM = pl.BlockSpec(memory_space=pltpu.VMEM)
MIB = 2**20


def first_gather(rows, arrays):
    weight_gate, weight_up, weight_down, norm_train = arrays[0], arrays[3], arrays[6], arrays[9]
    own = (weight_down.shape[1], weight_down.shape[0])
    shapes = [
        (weight_gate.shape[1], weight_gate.shape[0] * rows),
        (weight_up.shape[1], weight_up.shape[0] * rows),
        own,
        (3, own[0], sum(cuts(DOWN, own[1])[EARLY - 1])),
    ]
    lanes = -(-norm_train.shape[1] // 128) * 128
    count = len(UNITS[0]) + len(UNITS[1])
    dma = pltpu.SemaphoreType.DMA
    return pl.pallas_call(
        first_kernel,
        out_shape=[pltpu.VMEM(s, jnp.bfloat16) for s in shapes] + [pltpu.VMEM((1, lanes), jnp.float32)],
        in_specs=[HBM] * len(arrays),
        out_specs=[VMEM] * 5,
        scratch_shapes=[pltpu.VMEM(a.shape, a.dtype) for a in arrays]
        + [
            dma((count + 14,)),
            dma((3, count)), dma((3, count)), dma((4, count)), dma((4, count)),
            dma((3, EARLY)), dma((3, EARLY)),
        ],
        compiler_params=pltpu.CompilerParams(collective_id=0, has_side_effects=True, vmem_limit_bytes=44 * MIB),
    )(*arrays)


def second_gather(rows, model, own, early, part, token):
    dma = pltpu.SemaphoreType.DMA
    count = len(DOWN)
    small = model - 1 + 3 + 4
    return pl.pallas_call(
        functools.partial(second_kernel, model),
        out_shape=[
            pltpu.VMEM((own.shape[0] * rows, own.shape[1]), jnp.bfloat16),
            pltpu.VMEM((rows, model, *part.shape), jnp.float32),
        ],
        in_specs=[VMEM, VMEM, VMEM, HBM],
        out_specs=[VMEM, VMEM],
        scratch_shapes=[
            dma((3, count)), dma((3, count)), dma((4, count)), dma((4, count)), dma((small,)), dma((small,)),
            pltpu.SemaphoreType.REGULAR,
        ],
        compiler_params=pltpu.CompilerParams(collective_id=1, has_side_effects=True, vmem_limit_bytes=4 * MIB),
    )(own, early, part, token)


def write_kernel(g, u, og, ou, token, sems):
    copies = [pltpu.make_async_copy(s, t, sems.at[i]) for i, (s, t) in enumerate(((g, og), (u, ou)))]
    for c in copies:
        c.start()
    token[...] = jnp.zeros(token.shape, token.dtype)
    for c in copies:
        c.wait()


def written(gate, up):
    return pl.pallas_call(
        write_kernel,
        out_shape=[jax.ShapeDtypeStruct(a.shape, a.dtype) for a in (gate, up)]
        + [jax.ShapeDtypeStruct((8, 128), jnp.float32)],
        in_specs=[VMEM] * 2,
        out_specs=[HBM] * 2 + [VMEM],
        scratch_shapes=[pltpu.SemaphoreType.DMA((2,))],
        compiler_params=pltpu.CompilerParams(vmem_limit_bytes=MIB),
    )(gate, up)


def last_kernel(size, d, norm, od, out, packed_norm, sems):
    c = pltpu.make_async_copy(d, od, sems.at[0])
    c.start()
    rows, model, _, lanes = norm.shape
    parts = [norm[r, m][:, :size] for r in range(rows) for m in range(model)]
    group = lanes // size
    packed = [jnp.concatenate(parts[i : i + group], axis=1) for i in range(0, len(parts), group)]
    packed_norm[...] = jnp.concatenate(packed, axis=0).astype(out.dtype)
    small = pltpu.make_async_copy(packed_norm, out, sems.at[1])
    small.start()
    small.wait()
    c.wait()


def last_written(size, down, norm):
    rows, model, _, lanes = norm.shape
    packed = (rows * model * size // lanes, lanes)
    return pl.pallas_call(
        functools.partial(last_kernel, size),
        out_shape=[jax.ShapeDtypeStruct(down.shape, down.dtype), jax.ShapeDtypeStruct(packed, jnp.bfloat16)],
        in_specs=[VMEM] * 2,
        out_specs=[HBM] * 2,
        scratch_shapes=[pltpu.VMEM(packed, jnp.bfloat16), pltpu.SemaphoreType.DMA((2,))],
        compiler_params=pltpu.CompilerParams(vmem_limit_bytes=MIB),
    )(down, norm)


def local_kernel(rows, model, *arrays):
    arrays = tuple(a.T if i in (1, 4, 7) else a for i, a in enumerate(arrays[:9])) + tuple(
        a.reshape(1, -1) for a in arrays[9:]
    )
    gate, up, own, early, part = first_gather(rows, arrays)
    gate, up, token = written(gate, up)
    down, norm = second_gather(rows, model, own, early, part, token)
    down, serve_norm = last_written(arrays[9].shape[1], down, norm)
    return gate, up, down, serve_norm.reshape(-1)


def merge(weight, low, high):
    full = weight.astype(jnp.float32) + mix_rate * jnp.dot(low, high, preferred_element_type=jnp.float32)
    return full.astype(jnp.bfloat16).T


def local_plain(*arrays):
    gate, up, down = merge(*arrays[:3]), merge(*arrays[3:6]), merge(*arrays[6:9])
    return (
        lax.all_gather(gate, "rows", axis=1, tiled=True),
        lax.all_gather(up, "rows", axis=1, tiled=True),
        lax.all_gather(down, "rows", axis=0, tiled=True),
        lax.all_gather((arrays[9] + arrays[10]).astype(jnp.bfloat16), ("rows", "model"), axis=0, tiled=True),
    )


def solution(mesh):
    rows, model = mesh.shape["rows"], mesh.shape["model"]
    local = functools.partial(local_kernel, rows, model) if rows == 2 * SIDE * SIDE else local_plain
    in_specs = (
        P("rows", "model"), P("rows", None), P(None, "model"),
        P("rows", "model"), P("rows", None), P(None, "model"),
        P("model", "rows"), P("model", None), P(None, "rows"),
        P(("rows", "model")), P(("rows", "model")),
    )
    out_specs = (P("model", None), P("model", None), P(None, "model"), P())
    return jax.shard_map(local, mesh=mesh, in_specs=in_specs, out_specs=out_specs, check_vma=False)
```

```python
import functools

import jax
import jax.numpy as jnp
from jax import lax
from jax.experimental import pallas as pl
from jax.experimental.pallas import tpu as pltpu
from jax.sharding import PartitionSpec as P

mix_rate = 0.5
MESH = pl.DeviceIdType.MESH
UNITS = ((1, 1, 3, 3, 4, 4), (4, 4, 3, 3, 1, 1))
DOWN = (4, 4, 3, 3, 1, 1)
EARLY = 4
SIDE = 2


def cuts(parts, size):
    whole = sum(parts)
    return [(sum(parts[:i]) * size // whole, parts[i] * size // whole) for i in range(len(parts))]


class Place:
    def __init__(self):
        self.me = me = lax.axis_index("rows")
        self.core = core = lax.rem(me, 2)
        x = lax.rem(me // 2, SIDE)
        y = me // (2 * SIDE)

        def device(y, x, core):
            return (y * SIDE + x) * 2 + core

        self.near_x, self.near_y = device(y, 1 - x, core), device(1 - y, x, core)
        self.far = device(1 - y, 1 - x, core)
        self.pair = device(y, x, 1 - core)
        self.pair_x, self.pair_y = device(y, 1 - x, 1 - core), device(1 - y, x, 1 - core)
        self.pair_far = device(1 - y, 1 - x, 1 - core)


def remote(src, dst, send, recv, target):
    return pltpu.make_async_remote_copy(
        src_ref=src, dst_ref=dst, send_sem=send, recv_sem=recv,
        device_id=target if isinstance(target, dict) else {"rows": target}, device_id_type=MESH,
    )


def first_kernel(model, *refs):
    sources, (og, ou, own, early, norm), refs = refs[:11], refs[11:16], refs[16:]
    held, refs = refs[:11], refs[11:]
    wg, lg, hg, wu, lu, hu, wd, ld, hd, nt, ns = held
    fetch_sem, link_send, link_recv, pair_send, pair_recv, early_send, early_recv, norm_send, norm_recv, part = refs
    at = Place()
    me, near_x, near_y, far, pair = at.me, at.near_x, at.near_y, at.far, at.pair
    depth = lax.axis_index("model")
    chip = me // 2

    barrier = pltpu.get_barrier_semaphore()
    for other in (near_x, near_y, pair):
        pl.semaphore_signal(barrier, inc=1, device_id={"rows": other}, device_id_type=MESH)

    @pl.when(at.core == 1)
    def _():
        for step in range(1, model):
            pl.semaphore_signal(barrier, inc=1, device_id={"model": lax.rem(depth + step, model)}, device_id_type=MESH)

    outs = (og, ou)
    fetches = {}

    def fetch(key, i, *cut):
        fetches[key] = pltpu.make_async_copy(
            sources[i].at[cut] if cut else sources[i], held[i].at[cut] if cut else held[i],
            fetch_sem.at[len(fetches)],
        )

    short, short_down = wg.shape[0], wd.shape[1]
    units = [(a, *cut) for a in range(2) for cut in cuts(UNITS[a], wg.shape[1])]
    count = len(units)
    work = units + [(2, *cut) for cut in cuts((1, 1, 1, 1), wd.shape[0])]
    whole = slice(None)

    for u, (a, start, size) in enumerate(work):
        if start == 0:
            fetch(("low", a), 3 * a + 1)
            if a < 2:
                fetch(("high", a), 3 * a + 2, whole, pl.ds(0, size))
            else:
                fetch(("high", a), 3 * a + 2)
        if a < 2:
            fetch(u, 3 * a, whole, pl.ds(start, size))
        else:
            fetch(u, 3 * a, pl.ds(start, size), whole)
        if start == 0 and a < 2:
            fetch(("rest", a), 3 * a + 2, whole, pl.ds(size, wg.shape[1] - size))
    fetch("train", 9)
    fetch("step", 10)
    for f in fetches.values():
        f.start()

    def place(u, owner):
        a, start, size = units[u]
        return outs[a].at[pl.ds(start, size), pl.ds(pl.multiple_of(owner * short, short), short)]

    def compute(u):
        a, start, size = work[u]
        if start == 0:
            fetches["low", a].wait()
            fetches["high", a].wait()
        elif a < 2 and work[u - 1][1] == 0:
            fetches["rest", a].wait()
        fetches[u].wait()
        cut = slice(start, start + size)
        if a < 2:
            w, low, high = ((wg, lg, hg), (wu, lu, hu))[a]
            weight, low, high = w[:, cut], low[...], high[:, cut]
        else:
            weight, low, high = wd[cut, :], ld[:, cut], hd[...]
        merged = weight.astype(jnp.float32) + mix_rate * lax.dot_general(
            low, high, (((0,), (0,)), ((), ())), preferred_element_type=jnp.float32
        )
        merged = merged.astype(jnp.bfloat16).T
        if a < 2:
            place(u, me)[...] = merged
        else:
            own[:, cut] = merged

    def copy(u, owner, send, recv, target):
        return remote(place(u, owner), place(u, owner), send, recv, target)

    def link(lane, u, owner, target):
        return copy(u, owner, link_send.at[lane, u], link_recv.at[lane, u], target)

    def across(lane, u, owner):
        return copy(u, owner, pair_send.at[lane, u], pair_recv.at[lane, u], pair)

    pieces = cuts(DOWN, own.shape[1])[:EARLY]

    def ahead(lane, k, src, target):
        cut = (whole, pl.ds(*pieces[k]))
        src = own.at[cut] if src is None else early.at[(src, *cut)]
        return remote(src, early.at[(lane, *cut)], early_send.at[lane, k], early_recv.at[lane, k], target)

    def send_own(u):
        link(0, u, me, near_x).start()
        link(1, u, me, near_y).start()
        across(3, u, me).start()

    compute(0)
    pl.semaphore_wait(barrier, 3 + at.core * (model - 1))
    for u in range(1, count + 1):
        compute(u)
        send_own(u - 1)
    for u in range(count + 1, len(work)):
        compute(u)
    fetches["train"].wait()
    fetches["step"].wait()
    part[...] = jnp.zeros(part.shape, part.dtype)
    part[:, : nt.shape[1]] = nt[...] + ns[...]

    @pl.when(at.core == 1)
    def _():
        norm[chip, depth, 1] = part[...]

    def norm_copy(slot, ref, target):
        return remote(ref, ref, norm_send.at[slot], norm_recv.at[slot], target)

    def norm_part():
        return remote(part, norm.at[chip, depth, 0], norm_send.at[0], norm_recv.at[0], pair)

    def norm_deep(step, send):
        return norm_copy(
            step, norm.at[chip, depth if send else lax.rem(depth + model - step, model)],
            {"model": lax.rem(depth + step, model)},
        )

    def norm_wide(lane, owner, target):
        return norm_copy(model + lane, norm.at[owner // 2], target)

    def norm_whole():
        return norm_copy(model + 3, norm, pair)

    def norm_step(u):
        if u == 1:
            norm_part().wait_recv()
            for step in range(1, model):
                norm_deep(step, True).start()
        if u == 2:
            for step in range(1, model):
                norm_deep(step, False).wait_recv()
            norm_wide(0, me, near_x).start()
            norm_wide(1, me, near_y).start()
        if u == 3:
            norm_wide(0, near_x, near_x).wait_recv()
            norm_wide(1, near_y, near_y).wait_recv()
            norm_wide(2, near_x, near_y).start()
        if u == 4:
            norm_wide(2, far, near_y).wait_recv()
            norm_whole().start()

    for u in range(count):
        link(0, u, near_x, near_x).wait_recv()
        if u % 2 == 0:
            link(2, u, near_x, near_y).start()
        across(0, u, near_x).start()
        link(1, u, near_y, near_y).wait_recv()
        if u % 2 == 1:
            link(2, u, near_y, near_x).start()
        across(1, u, near_y).start()
        if u == 0:
            pl.when(at.core == 0)(lambda: norm_part().start())
        if 1 <= u <= 4:
            pl.when(at.core == 1)(functools.partial(norm_step, u))

    @pl.when(at.core == 1)
    def _():
        for k in range(EARLY):
            ahead(0, k, None, near_x).start()
            ahead(1, k, None, near_y).start()

    for u in range(count):
        link(2, u, far, near_x).wait_recv()
        across(2, u, far).start()

    @pl.when(at.core == 1)
    def _():
        for k in range(EARLY):
            ahead(0, k, None, near_x).wait_recv()
            if k % 2 == 0:
                ahead(2, k, 0, near_y).start()
            ahead(1, k, None, near_y).wait_recv()
            if k % 2 == 1:
                ahead(2, k, 1, near_x).start()

    @pl.when(at.core == 0)
    def _():
        norm_part().wait_send()
        norm_whole().wait_recv()

    for u in range(count):
        link(0, u, me, near_x).wait_send()
        link(1, u, me, near_y).wait_send()
        link(2, u, near_x, near_x).wait_send()
        for lane, mine, theirs in ((3, me, pair), (0, near_x, at.pair_x), (1, near_y, at.pair_y), (2, far, at.pair_far)):
            across(lane, u, mine).wait_send()
            across(lane, u, theirs).wait_recv()

    @pl.when(at.core == 1)
    def _():
        for k in range(EARLY):
            ahead(0, k, None, near_x).wait_send()
            ahead(1, k, None, near_y).wait_send()
            ahead(2, k, k % 2, near_x).wait_send()
            ahead(2, k, None, near_x).wait_recv()
        for step in range(1, model):
            norm_deep(step, True).wait_send()
        norm_wide(0, me, near_x).wait_send()
        norm_wide(1, me, near_y).wait_send()
        norm_wide(2, near_x, near_y).wait_send()
        norm_whole().wait_send()


def second_kernel(own, early, token, down, link_send, link_recv, pair_send, pair_recv, ready):
    at = Place()
    me, near_x, near_y, far, pair = at.me, at.near_x, at.near_y, at.far, at.pair
    short = own.shape[0]
    pieces = cuts(DOWN, own.shape[1])

    barrier = pltpu.get_barrier_semaphore()
    for other in (near_x, near_y):
        pl.semaphore_signal(barrier, inc=1, device_id={"rows": other}, device_id_type=MESH)
    pl.semaphore_wait(barrier, 2 + at.core)

    def cut(k):
        return slice(None), pl.ds(*pieces[k])

    def band(owner):
        return pl.ds(pl.multiple_of(owner * short, short), short)

    def place(k, owner):
        return down.at[band(owner), pl.ds(*pieces[k])]

    def link(lane, k, src, owner, target):
        return remote(src, place(k, owner), link_send.at[lane, k], link_recv.at[lane, k], target)

    def across(lane, k, src, owner):
        return remote(src, place(k, owner), pair_send.at[lane, k], pair_recv.at[lane, k], pair)

    def gather(first):
        late, everything = range(first, len(pieces)), range(len(pieces))
        for k in late:
            link(0, k, own.at[cut(k)], me, near_x).start()
            link(1, k, own.at[cut(k)], me, near_y).start()

        def over():
            for k in everything:
                across(3, k, own.at[cut(k)], me).start()
            for k in range(first):
                for lane, owner in enumerate((near_x, near_y, far)):
                    across(lane, k, early.at[(lane, *cut(k))], owner).start()

        if first:
            over()
        down[band(me), :] = own[...]
        if first:
            end = sum(pieces[first - 1])
            for lane, owner in enumerate((near_x, near_y, far)):
                down[band(owner), :end] = early[lane]
        for k in late:
            link(0, k, place(k, near_x), near_x, near_x).wait_recv()
            if k % 2 == 0:
                link(2, k, place(k, near_x), near_x, near_y).start()
            link(1, k, place(k, near_y), near_y, near_y).wait_recv()
            if k % 2 == 1:
                link(2, k, place(k, near_y), near_y, near_x).start()
        if not first:
            pl.semaphore_wait(ready, 1)
            over()
        for k in late:
            across(0, k, place(k, near_x), near_x).start()
            across(1, k, place(k, near_y), near_y).start()
        for k in late:
            link(2, k, place(k, far), far, near_x).wait_recv()
            across(2, k, place(k, far), far).start()

        for k in late:
            link(0, k, own.at[cut(k)], me, near_x).wait_send()
            link(1, k, own.at[cut(k)], me, near_y).wait_send()
            link(2, k, place(k, near_x), near_x, near_x).wait_send()
        for k in everything:
            for lane, mine, theirs in ((3, me, pair), (0, near_x, at.pair_x), (1, near_y, at.pair_y), (2, far, at.pair_far)):
                across(lane, k, place(k, mine), mine).wait_send()
                across(lane, k, place(k, theirs), theirs).wait_recv()

    @pl.when(at.core == 0)
    def _():
        pl.semaphore_signal(barrier, inc=1, device_id={"rows": pair}, device_id_type=MESH)
        gather(0)

    @pl.when(at.core == 1)
    def _():
        pl.semaphore_signal(ready, inc=1, device_id={"rows": pair}, device_id_type=MESH)
        gather(EARLY)


HBM = pl.BlockSpec(memory_space=pltpu.HBM)
VMEM = pl.BlockSpec(memory_space=pltpu.VMEM)
MIB = 2**20


def first_gather(rows, model, arrays):
    weight_gate, weight_up, weight_down, norm_train = arrays[0], arrays[3], arrays[6], arrays[9]
    own = (weight_down.shape[1], weight_down.shape[0])
    shapes = [
        (weight_gate.shape[1], weight_gate.shape[0] * rows),
        (weight_up.shape[1], weight_up.shape[0] * rows),
        own,
        (3, own[0], sum(cuts(DOWN, own[1])[EARLY - 1])),
    ]
    lanes = -(-norm_train.shape[1] // 128) * 128
    count = len(UNITS[0]) + len(UNITS[1])
    dma = pltpu.SemaphoreType.DMA
    return pl.pallas_call(
        functools.partial(first_kernel, model),
        out_shape=[pltpu.VMEM(s, jnp.bfloat16) for s in shapes] + [pltpu.VMEM((rows // 2, model, 2, 1, lanes), jnp.float32)],
        in_specs=[HBM] * len(arrays),
        out_specs=[VMEM] * 5,
        scratch_shapes=[pltpu.VMEM(a.shape, a.dtype) for a in arrays]
        + [
            dma((count + 14,)),
            dma((3, count)), dma((3, count)), dma((4, count)), dma((4, count)),
            dma((3, EARLY)), dma((3, EARLY)), dma((model + 4,)), dma((model + 4,)),
            pltpu.VMEM((1, lanes), jnp.float32),
        ],
        compiler_params=pltpu.CompilerParams(collective_id=0, has_side_effects=True, vmem_limit_bytes=44 * MIB),
    )(*arrays)


def second_gather(rows, own, early, token):
    dma = pltpu.SemaphoreType.DMA
    count = len(DOWN)
    return pl.pallas_call(
        second_kernel,
        out_shape=pltpu.VMEM((own.shape[0] * rows, own.shape[1]), jnp.bfloat16),
        in_specs=[VMEM, VMEM, HBM],
        out_specs=VMEM,
        scratch_shapes=[
            dma((3, count)), dma((3, count)), dma((4, count)), dma((4, count)), pltpu.SemaphoreType.REGULAR,
        ],
        compiler_params=pltpu.CompilerParams(collective_id=1, has_side_effects=True, vmem_limit_bytes=4 * MIB),
    )(own, early, token)


def write_kernel(size, g, u, norm, og, ou, out, token, packed_norm, sems):
    copies = [pltpu.make_async_copy(s, t, sems.at[i]) for i, (s, t) in enumerate(((g, og), (u, ou), (packed_norm, out)))]
    copies[0].start()
    copies[1].start()
    token[...] = jnp.zeros(token.shape, token.dtype)
    chips, model, cores, _, lanes = norm.shape
    parts = [norm[r, m, c][:, :size] for r in range(chips) for c in range(cores) for m in range(model)]
    group = lanes // size
    packed = [jnp.concatenate(parts[i : i + group], axis=1) for i in range(0, len(parts), group)]
    packed_norm[...] = jnp.concatenate(packed, axis=0).astype(out.dtype)
    copies[2].start()
    for c in copies:
        c.wait()


def written(size, gate, up, norm):
    chips, model, cores, _, lanes = norm.shape
    packed = (chips * model * cores * size // lanes, lanes)
    return pl.pallas_call(
        functools.partial(write_kernel, size),
        out_shape=[jax.ShapeDtypeStruct(s, jnp.bfloat16) for s in (gate.shape, up.shape, packed)]
        + [jax.ShapeDtypeStruct((8, 128), jnp.float32)],
        in_specs=[VMEM] * 3,
        out_specs=[HBM] * 3 + [VMEM],
        scratch_shapes=[pltpu.VMEM(packed, jnp.bfloat16), pltpu.SemaphoreType.DMA((3,))],
        compiler_params=pltpu.CompilerParams(vmem_limit_bytes=MIB),
    )(gate, up, norm)


def last_kernel(d, od, sem):
    c = pltpu.make_async_copy(d, od, sem)
    c.start()
    c.wait()


def last_written(down):
    return pl.pallas_call(
        last_kernel,
        out_shape=jax.ShapeDtypeStruct(down.shape, down.dtype),
        in_specs=[VMEM],
        out_specs=HBM,
        scratch_shapes=[pltpu.SemaphoreType.DMA(())],
        compiler_params=pltpu.CompilerParams(vmem_limit_bytes=MIB),
    )(down)


def local_kernel(rows, model, *arrays):
    arrays = tuple(a.T if i in (1, 4, 7) else a for i, a in enumerate(arrays[:9])) + tuple(
        a.reshape(1, -1) for a in arrays[9:]
    )
    gate, up, own, early, norm = first_gather(rows, model, arrays)
    gate, up, serve_norm, token = written(arrays[9].shape[1], gate, up, norm)
    down = last_written(second_gather(rows, own, early, token))
    return gate, up, down, serve_norm.reshape(-1)


def merge(weight, low, high):
    full = weight.astype(jnp.float32) + mix_rate * jnp.dot(low, high, preferred_element_type=jnp.float32)
    return full.astype(jnp.bfloat16).T


def local_plain(*arrays):
    gate, up, down = merge(*arrays[:3]), merge(*arrays[3:6]), merge(*arrays[6:9])
    return (
        lax.all_gather(gate, "rows", axis=1, tiled=True),
        lax.all_gather(up, "rows", axis=1, tiled=True),
        lax.all_gather(down, "rows", axis=0, tiled=True),
        lax.all_gather((arrays[9] + arrays[10]).astype(jnp.bfloat16), ("rows", "model"), axis=0, tiled=True),
    )


def solution(mesh):
    rows, model = mesh.shape["rows"], mesh.shape["model"]
    local = functools.partial(local_kernel, rows, model) if rows == 2 * SIDE * SIDE else local_plain
    in_specs = (
        P("rows", "model"), P("rows", None), P(None, "model"),
        P("rows", "model"), P("rows", None), P(None, "model"),
        P("model", "rows"), P("model", None), P(None, "rows"),
        P(("rows", "model")), P(("rows", "model")),
    )
    out_specs = (P("model", None), P("model", None), P(None, "model"), P())
    return jax.shard_map(local, mesh=mesh, in_specs=in_specs, out_specs=out_specs, check_vma=False)
```

```python
import functools

import jax
import jax.numpy as jnp
from jax import lax
from jax.experimental import pallas as pl
from jax.experimental.pallas import tpu as pltpu
from jax.sharding import PartitionSpec as P

mix_rate = 0.5
MESH = pl.DeviceIdType.MESH
UNITS = ((1, 1, 3, 3, 4, 4), (4, 4, 3, 3, 1, 1))
DOWN = (4, 4, 3, 3, 1, 1)
EARLY = 4
SIDE = 2


def cuts(parts, size):
    whole = sum(parts)
    return [(sum(parts[:i]) * size // whole, parts[i] * size // whole) for i in range(len(parts))]


class Place:
    def __init__(self):
        self.me = me = lax.axis_index("rows")
        self.core = core = lax.rem(me, 2)
        x = lax.rem(me // 2, SIDE)
        y = me // (2 * SIDE)

        def device(y, x, core):
            return (y * SIDE + x) * 2 + core

        self.near_x, self.near_y = device(y, 1 - x, core), device(1 - y, x, core)
        self.far = device(1 - y, 1 - x, core)
        self.pair = device(y, x, 1 - core)
        self.pair_x, self.pair_y = device(y, 1 - x, 1 - core), device(1 - y, x, 1 - core)
        self.pair_far = device(1 - y, 1 - x, 1 - core)


def remote(src, dst, send, recv, target):
    return pltpu.make_async_remote_copy(
        src_ref=src, dst_ref=dst, send_sem=send, recv_sem=recv,
        device_id=target if isinstance(target, dict) else {"rows": target}, device_id_type=MESH,
    )


def sent(ref, sem, other):
    remote(ref, ref, sem, sem, other).wait_send()


def came(ref, sem, other):
    remote(ref, ref, sem, sem, other).wait_recv()


def first_kernel(model, *refs):
    sources, (og, ou, own, early, norm), refs = refs[:11], refs[11:16], refs[16:]
    held, refs = refs[:11], refs[11:]
    wg, lg, hg, wu, lu, hu, wd, ld, hd, nt, ns = held
    fetch_sem, link_send, link_recv, rest_recv, far_recv, pair_send, pair_recv, early_send, early_recv, norm_send, norm_recv, part = refs
    at = Place()
    me, near_x, near_y, far, pair = at.me, at.near_x, at.near_y, at.far, at.pair
    depth = lax.axis_index("model")
    chip = me // 2

    barrier = pltpu.get_barrier_semaphore()
    for other in (near_x, near_y, pair):
        pl.semaphore_signal(barrier, inc=1, device_id={"rows": other}, device_id_type=MESH)

    @pl.when(at.core == 1)
    def _():
        for step in range(1, model):
            pl.semaphore_signal(barrier, inc=1, device_id={"model": lax.rem(depth + step, model)}, device_id_type=MESH)

    outs = (og, ou)
    fetches = {}

    def fetch(key, i, *cut):
        fetches[key] = pltpu.make_async_copy(
            sources[i].at[cut] if cut else sources[i], held[i].at[cut] if cut else held[i],
            fetch_sem.at[len(fetches)],
        )

    short, short_down = wg.shape[0], wd.shape[1]
    units = [(a, *cut) for a in range(2) for cut in cuts(UNITS[a], wg.shape[1])]
    count = len(units)
    work = units + [(2, *cut) for cut in cuts((1, 1, 1, 1), wd.shape[0])]
    whole = slice(None)

    first, rest = sum(units[1][1:]), wg.shape[1]
    fetch("low", 1)
    fetch("high", 2, whole, pl.ds(0, first))
    fetch("gate", 0, whole, pl.ds(0, first))
    fetch("high_rest", 2, whole, pl.ds(first, rest - first))
    fetch("gate_rest", 0, whole, pl.ds(first, rest - first))
    for a in (1, 2):
        for i in (1, 2, 0):
            fetch((a, i), 3 * a + i)
    fetch("train", 9)
    fetch("step", 10)
    for f in fetches.values():
        f.start()

    def place(u, owner):
        a, start, size = units[u]
        return outs[a].at[pl.ds(start, size), pl.ds(pl.multiple_of(owner * short, short), short)]

    def compute(u):
        a, start, size = work[u]
        if u == 0:
            needed = ("low", "high", "gate")
        elif u == 2:
            needed = ("high_rest", "gate_rest")
        elif a and start == 0:
            needed = [(a, i) for i in range(3)]
        else:
            needed = ()
        for key in needed:
            fetches[key].wait()
        cut = slice(start, start + size)
        if a < 2:
            w, low, high = ((wg, lg, hg), (wu, lu, hu))[a]
            weight, low, high = w[:, cut], low[...], high[:, cut]
        else:
            weight, low, high = wd[cut, :], ld[:, cut], hd[...]
        merged = weight.astype(jnp.float32) + mix_rate * lax.dot_general(
            low, high, (((0,), (0,)), ((), ())), preferred_element_type=jnp.float32
        )
        merged = merged.astype(jnp.bfloat16).T
        if a < 2:
            place(u, me)[...] = merged
        else:
            own[:, cut] = merged

    def copy(u, owner, send, recv, target):
        return remote(place(u, owner), place(u, owner), send, recv, target)

    far_groups = [list(range(len(UNITS[0]))), list(range(len(UNITS[0]), count - 2)), [count - 2], [count - 1]]

    def link(lane, u, owner, target):
        if lane == 2:
            recv = far_recv.at[next(g for g, group in enumerate(far_groups) if u in group)]
        else:
            recv = link_recv.at[u] if lane == u % 2 else rest_recv.at[units[u][0]]
        return copy(u, owner, link_send, recv, target)

    def across(lane, u, owner):
        return copy(u, owner, pair_send, pair_recv, pair)

    def sized(group):
        return og.at[pl.ds(0, sum(units[u][2] for u in group)), pl.ds(0, short)]

    pieces = cuts(DOWN, own.shape[1])[:EARLY]

    def ahead(lane, k, src, target):
        cut = (whole, pl.ds(*pieces[k]))
        src = own.at[cut] if src is None else early.at[(src, *cut)]
        recv = early_recv.at[k if lane == k % 2 else EARLY]
        return remote(src, early.at[(lane, *cut)], early_send, recv, target)

    def send_own(u):
        link(0, u, me, near_x).start()
        link(1, u, me, near_y).start()
        across(3, u, me).start()

    compute(0)
    pl.semaphore_wait(barrier, 3 + at.core * (model - 1))
    for u in range(1, count + 1):
        compute(u)
        send_own(u - 1)
    for u in range(count + 1, len(work)):
        compute(u)
    fetches["train"].wait()
    fetches["step"].wait()
    part[...] = jnp.zeros(part.shape, part.dtype)
    part[:, : nt.shape[1]] = nt[...] + ns[...]

    @pl.when(at.core == 1)
    def _():
        norm[chip, depth, 1] = part[...]

    def norm_copy(kind, ref, target):
        return remote(ref, ref, norm_send.at[kind], norm_recv.at[kind], target)

    def norm_part():
        return remote(part, norm.at[chip, depth, 0], norm_send.at[4], norm_recv.at[4], pair)

    def norm_whole():
        return norm_copy(3, norm, pair)

    def norm_step(u):
        if u == 1:
            norm_part().wait_recv()
            for step in range(1, model):
                norm_copy(0, norm.at[chip, depth], {"model": lax.rem(depth + step, model)}).start()
        if u == 2:
            came(norm.at[chip, pl.ds(0, model - 1)], norm_recv.at[0], near_x)
            norm_copy(1, norm.at[chip], near_x).start()
            norm_copy(1, norm.at[chip], near_y).start()
        if u == 3:
            came(norm.at[pl.ds(0, 2)], norm_recv.at[1], near_x)
            norm_copy(2, norm.at[near_x // 2], near_y).start()
        if u == 4:
            came(norm.at[chip], norm_recv.at[2], near_y)
            norm_whole().start()

    for u in range(count):
        a, lane = units[u][0], u % 2
        owner, target = ((near_x, near_y), (near_y, near_x))[lane]
        link(lane, u, owner, owner).wait_recv()
        link(2, u, owner, target).start()
        across(lane, u, owner).start()
        if u == count - 1 or units[u + 1][0] > a:
            group = [v for v in range(count) if units[v][0] == a]
            came(sized(group), rest_recv.at[a], near_x)
            for v in group:
                across(1 - v % 2, v, (near_y, near_x)[v % 2]).start()
        if u == 0:
            pl.when(at.core == 0)(lambda: norm_part().start())
        if 1 <= u <= 4:
            pl.when(at.core == 1)(functools.partial(norm_step, u))

    @pl.when(at.core == 1)
    def _():
        for k in range(EARLY):
            ahead(0, k, None, near_x).start()
            ahead(1, k, None, near_y).start()

    for g, group in enumerate(far_groups):
        came(sized(group), far_recv.at[g], near_x)
        for u in group:
            across(2, u, far).start()

    @pl.when(at.core == 1)
    def _():
        for k in range(EARLY):
            owner, target = ((near_x, near_y), (near_y, near_x))[k % 2]
            ahead(k % 2, k, None, owner).wait_recv()
            ahead(2, k, k % 2, target).start()

    @pl.when(at.core == 0)
    def _():
        norm_part().wait_send()
        norm_whole().wait_recv()

    @pl.when(at.core == 1)
    def _():
        sent(norm.at[chip, pl.ds(0, model - 1)], norm_send.at[0], near_x)
        sent(norm.at[pl.ds(0, 2)], norm_send.at[1], near_x)
        sent(norm.at[chip], norm_send.at[2], near_y)
        sent(norm, norm_send.at[3], pair)
        sent(early, early_send, near_x)
        came(early.at[pl.ds(0, 2)], early_recv.at[EARLY], near_x)

    sent(og.at[:, pl.ds(0, 2 * 3 * short)], link_send, near_x)
    sent(og, pair_send, pair)
    came(og, pair_recv, pair)


def second_kernel(own, early, token, down, link_send, link_recv, rest_recv, far_recv, pair_send, pair_recv, ready):
    at = Place()
    me, near_x, near_y, far, pair = at.me, at.near_x, at.near_y, at.far, at.pair
    short = own.shape[0]
    pieces = cuts(DOWN, own.shape[1])

    barrier = pltpu.get_barrier_semaphore()
    for other in (near_x, near_y):
        pl.semaphore_signal(barrier, inc=1, device_id={"rows": other}, device_id_type=MESH)
    pl.semaphore_wait(barrier, 2 + at.core)

    def cut(k):
        return slice(None), pl.ds(*pieces[k])

    def band(owner):
        return pl.ds(pl.multiple_of(owner * short, short), short)

    def place(k, owner):
        return down.at[band(owner), pl.ds(*pieces[k])]

    def link(lane, k, src, owner, target):
        recv = far_recv.at[k] if lane == 2 else link_recv.at[k] if lane == k % 2 else rest_recv
        return remote(src, place(k, owner), link_send, recv, target)

    def across(lane, k, src, owner):
        return remote(src, place(k, owner), pair_send, pair_recv, pair)

    def gather(first):
        late, everything = range(first, len(pieces)), range(len(pieces))
        for k in late:
            link(0, k, own.at[cut(k)], me, near_x).start()
            link(1, k, own.at[cut(k)], me, near_y).start()

        def over():
            for k in everything:
                across(3, k, own.at[cut(k)], me).start()
            for k in range(first):
                for lane, owner in enumerate((near_x, near_y, far)):
                    across(lane, k, early.at[(lane, *cut(k))], owner).start()

        if first:
            over()
        down[band(me), :] = own[...]
        if first:
            end = sum(pieces[first - 1])
            for lane, owner in enumerate((near_x, near_y, far)):
                down[band(owner), :end] = early[lane]
        width = own.shape[1] - pieces[first][0]
        for k in late:
            owner, target = ((near_x, near_y), (near_y, near_x))[k % 2]
            link(k % 2, k, place(k, owner), owner, owner).wait_recv()
            link(2, k, place(k, owner), owner, target).start()
        if not first:
            pl.semaphore_wait(ready, 1)
            over()
        came(down.at[pl.ds(0, short), pl.ds(0, width)], rest_recv, near_x)
        for k in late:
            across(0, k, place(k, near_x), near_x).start()
            across(1, k, place(k, near_y), near_y).start()
        for k in late:
            link(2, k, place(k, far), far, near_x).wait_recv()
            across(2, k, place(k, far), far).start()

        sent(down.at[pl.ds(0, 3 * short), pl.ds(0, width)], link_send, near_x)
        sent(down.at[pl.ds(0, 4 * short), :], pair_send, pair)
        came(down.at[pl.ds(0, 4 * short), :], pair_recv, pair)

    @pl.when(at.core == 0)
    def _():
        pl.semaphore_signal(barrier, inc=1, device_id={"rows": pair}, device_id_type=MESH)
        gather(0)

    @pl.when(at.core == 1)
    def _():
        pl.semaphore_signal(ready, inc=1, device_id={"rows": pair}, device_id_type=MESH)
        gather(EARLY)


HBM = pl.BlockSpec(memory_space=pltpu.HBM)
VMEM = pl.BlockSpec(memory_space=pltpu.VMEM)
MIB = 2**20


def first_gather(rows, model, arrays):
    weight_gate, weight_up, weight_down, norm_train = arrays[0], arrays[3], arrays[6], arrays[9]
    own = (weight_down.shape[1], weight_down.shape[0])
    shapes = [
        (weight_gate.shape[1], weight_gate.shape[0] * rows),
        (weight_up.shape[1], weight_up.shape[0] * rows),
        own,
        (3, own[0], sum(cuts(DOWN, own[1])[EARLY - 1])),
    ]
    lanes = -(-norm_train.shape[1] // 128) * 128
    count = len(UNITS[0]) + len(UNITS[1])
    dma = pltpu.SemaphoreType.DMA
    return pl.pallas_call(
        functools.partial(first_kernel, model),
        out_shape=[pltpu.VMEM(s, jnp.bfloat16) for s in shapes] + [pltpu.VMEM((rows // 2, model, 2, 1, lanes), jnp.float32)],
        in_specs=[HBM] * len(arrays),
        out_specs=[VMEM] * 5,
        scratch_shapes=[pltpu.VMEM(a.shape, a.dtype) for a in arrays]
        + [
            dma((13,)),
            dma(()), dma((count,)), dma((2,)), dma((4,)), dma(()), dma(()),
            dma(()), dma((EARLY + 1,)), dma((5,)), dma((5,)),
            pltpu.VMEM((1, lanes), jnp.float32),
        ],
        compiler_params=pltpu.CompilerParams(collective_id=0, has_side_effects=True, vmem_limit_bytes=44 * MIB),
    )(*arrays)


def second_gather(rows, own, early, token):
    dma = pltpu.SemaphoreType.DMA
    count = len(DOWN)
    return pl.pallas_call(
        second_kernel,
        out_shape=pltpu.VMEM((own.shape[0] * rows, own.shape[1]), jnp.bfloat16),
        in_specs=[VMEM, VMEM, HBM],
        out_specs=VMEM,
        scratch_shapes=[
            dma(()), dma((count,)), dma(()), dma((count,)), dma(()), dma(()), pltpu.SemaphoreType.REGULAR,
        ],
        compiler_params=pltpu.CompilerParams(collective_id=1, has_side_effects=True, vmem_limit_bytes=4 * MIB),
    )(own, early, token)


def write_kernel(size, g, u, norm, og, ou, out, token, packed_norm, sems):
    copies = [pltpu.make_async_copy(s, t, sems.at[i]) for i, (s, t) in enumerate(((g, og), (u, ou), (packed_norm, out)))]
    copies[0].start()
    copies[1].start()
    token[...] = jnp.zeros(token.shape, token.dtype)
    chips, model, cores, _, lanes = norm.shape
    parts = [norm[r, m, c][:, :size] for r in range(chips) for c in range(cores) for m in range(model)]
    group = lanes // size
    packed = [jnp.concatenate(parts[i : i + group], axis=1) for i in range(0, len(parts), group)]
    packed_norm[...] = jnp.concatenate(packed, axis=0).astype(out.dtype)
    copies[2].start()
    for c in copies:
        c.wait()


def written(size, gate, up, norm):
    chips, model, cores, _, lanes = norm.shape
    packed = (chips * model * cores * size // lanes, lanes)
    return pl.pallas_call(
        functools.partial(write_kernel, size),
        out_shape=[jax.ShapeDtypeStruct(s, jnp.bfloat16) for s in (gate.shape, up.shape, packed)]
        + [jax.ShapeDtypeStruct((8, 128), jnp.float32)],
        in_specs=[VMEM] * 3,
        out_specs=[HBM] * 3 + [VMEM],
        scratch_shapes=[pltpu.VMEM(packed, jnp.bfloat16), pltpu.SemaphoreType.DMA((3,))],
        compiler_params=pltpu.CompilerParams(vmem_limit_bytes=MIB),
    )(gate, up, norm)


def last_kernel(d, od, sem):
    c = pltpu.make_async_copy(d, od, sem)
    c.start()
    c.wait()


def last_written(down):
    return pl.pallas_call(
        last_kernel,
        out_shape=jax.ShapeDtypeStruct(down.shape, down.dtype),
        in_specs=[VMEM],
        out_specs=HBM,
        scratch_shapes=[pltpu.SemaphoreType.DMA(())],
        compiler_params=pltpu.CompilerParams(vmem_limit_bytes=MIB),
    )(down)


def local_kernel(rows, model, *arrays):
    arrays = tuple(a.T if i in (1, 4, 7) else a for i, a in enumerate(arrays[:9])) + tuple(
        a.reshape(1, -1) for a in arrays[9:]
    )
    gate, up, own, early, norm = first_gather(rows, model, arrays)
    gate, up, serve_norm, token = written(arrays[9].shape[1], gate, up, norm)
    down = last_written(second_gather(rows, own, early, token))
    return gate, up, down, serve_norm.reshape(-1)


def merge(weight, low, high):
    full = weight.astype(jnp.float32) + mix_rate * jnp.dot(low, high, preferred_element_type=jnp.float32)
    return full.astype(jnp.bfloat16).T


def local_plain(*arrays):
    gate, up, down = merge(*arrays[:3]), merge(*arrays[3:6]), merge(*arrays[6:9])
    return (
        lax.all_gather(gate, "rows", axis=1, tiled=True),
        lax.all_gather(up, "rows", axis=1, tiled=True),
        lax.all_gather(down, "rows", axis=0, tiled=True),
        lax.all_gather((arrays[9] + arrays[10]).astype(jnp.bfloat16), ("rows", "model"), axis=0, tiled=True),
    )


def solution(mesh):
    rows, model = mesh.shape["rows"], mesh.shape["model"]
    local = functools.partial(local_kernel, rows, model) if rows == 2 * SIDE * SIDE else local_plain
    in_specs = (
        P("rows", "model"), P("rows", None), P(None, "model"),
        P("rows", "model"), P("rows", None), P(None, "model"),
        P("model", "rows"), P("model", None), P(None, "rows"),
        P(("rows", "model")), P(("rows", "model")),
    )
    out_specs = (P("model", None), P("model", None), P(None, "model"), P())
    return jax.shard_map(local, mesh=mesh, in_specs=in_specs, out_specs=out_specs, check_vma=False)
```

```python
import functools

import jax
import jax.numpy as jnp
from jax import lax
from jax.experimental import pallas as pl
from jax.experimental.pallas import tpu as pltpu
from jax.sharding import PartitionSpec as P

mix_rate = 0.5
MESH = pl.DeviceIdType.MESH
UNITS = ((2, 2, 2, 2, 4, 4), (4, 4, 4, 4), (1, 1))
DOWN = (4, 4, 2, 2, 1, 1)
EARLY = 4
SIDE = 2


def cuts(parts, size):
    whole = sum(parts)
    return [(sum(parts[:i]) * size // whole, parts[i] * size // whole) for i in range(len(parts))]


def down_cuts(size):
    pieces = cuts(UNITS[2] + DOWN, size)
    head = len(UNITS[2])
    offset = pieces[head][0]
    return pieces[:head], [(start - offset, length) for start, length in pieces[head:]]


class Place:
    def __init__(self):
        self.me = me = lax.axis_index("rows")
        self.core = core = lax.rem(me, 2)
        x = lax.rem(me // 2, SIDE)
        y = me // (2 * SIDE)

        def device(y, x, core):
            return (y * SIDE + x) * 2 + core

        self.near_x, self.near_y = device(y, 1 - x, core), device(1 - y, x, core)
        self.far = device(1 - y, 1 - x, core)
        self.pair = device(y, x, 1 - core)
        self.pair_x, self.pair_y = device(y, 1 - x, 1 - core), device(1 - y, x, 1 - core)
        self.pair_far = device(1 - y, 1 - x, 1 - core)


def remote(src, dst, send, recv, target):
    return pltpu.make_async_remote_copy(
        src_ref=src, dst_ref=dst, send_sem=send, recv_sem=recv,
        device_id=target if isinstance(target, dict) else {"rows": target}, device_id_type=MESH,
    )


def sent(ref, sem, other):
    remote(ref, ref, sem, sem, other).wait_send()


def came(ref, sem, other):
    remote(ref, ref, sem, sem, other).wait_recv()


def first_kernel(model, *refs):
    sources, (og, ou, od, own, early, norm), refs = refs[:11], refs[11:17], refs[17:]
    held, refs = refs[:11], refs[11:]
    wg, lg, hg, wu, lu, hu, wd, ld, hd, nt, ns = held
    fetch_sem, link_send, link_recv, rest_recv, far_recv, pair_send, pair_recv, early_send, early_recv, norm_send, norm_recv, part = refs
    at = Place()
    me, near_x, near_y, far, pair = at.me, at.near_x, at.near_y, at.far, at.pair
    depth = lax.axis_index("model")
    chip = me // 2

    outs = (og, ou, od)
    fetches = {}

    def fetch(key, i, *cut):
        fetches[key] = pltpu.make_async_copy(
            sources[i].at[cut] if cut else sources[i], held[i].at[cut] if cut else held[i],
            fetch_sem.at[len(fetches)],
        )

    short, short_down = wg.shape[0], wd.shape[1]
    heads, pieces = down_cuts(wd.shape[0])
    offset = sum(heads[-1])
    units = [(a, *cut) for a in range(2) for cut in cuts(UNITS[a], wg.shape[1])] + [(2, *cut) for cut in heads]
    count = len(units)
    work = units + [(2, offset + start, size) for start, size in pieces]
    whole = slice(None)

    first, rest = sum(units[1][1:]), wg.shape[1]
    fetch("low", 1)
    fetch("high", 2, whole, pl.ds(0, first))
    fetch("gate", 0, whole, pl.ds(0, first))
    fetch("high_rest", 2, whole, pl.ds(first, rest - first))
    fetch("gate_rest", 0, whole, pl.ds(first, rest - first))
    for a in (1, 2):
        for i in (1, 2, 0):
            fetch((a, i), 3 * a + i)
    fetch("train", 9)
    fetch("step", 10)
    urgent = ("low", "high", "gate")
    for key in urgent:
        fetches[key].start()

    barrier = pltpu.get_barrier_semaphore()
    for other in (near_x, near_y, pair):
        pl.semaphore_signal(barrier, inc=1, device_id={"rows": other}, device_id_type=MESH)

    @pl.when(at.core == 1)
    def _():
        for step in range(1, model):
            pl.semaphore_signal(barrier, inc=1, device_id={"model": lax.rem(depth + step, model)}, device_id_type=MESH)

    def place(u, owner):
        a, start, size = units[u]
        if a == 2:
            return od.at[pl.ds(pl.multiple_of(owner * short_down, short_down), short_down), pl.ds(start, size)]
        return outs[a].at[pl.ds(start, size), pl.ds(pl.multiple_of(owner * short, short), short)]

    def compute(u):
        a, start, size = work[u]
        if u == 0:
            needed = ("low", "high", "gate")
        elif u == 2:
            needed = ("high_rest", "gate_rest")
        elif a and work[u - 1][0] < a:
            needed = [(a, i) for i in range(3)]
        else:
            needed = ()
        for key in needed:
            fetches[key].wait()
        cut = slice(start, start + size)
        if a < 2:
            w, low, high = ((wg, lg, hg), (wu, lu, hu))[a]
            weight, low, high = w[:, cut], low[...], high[:, cut]
        else:
            weight, low, high = wd[cut, :], ld[:, cut], hd[...]
        merged = weight.astype(jnp.float32) + mix_rate * lax.dot_general(
            low, high, (((0,), (0,)), ((), ())), preferred_element_type=jnp.float32
        )
        merged = merged.astype(jnp.bfloat16).T
        if u < count:
            place(u, me)[...] = merged
        else:
            own[:, start - offset : start - offset + size] = merged

    def copy(u, owner, send, recv, target):
        return remote(place(u, owner), place(u, owner), send, recv, target)

    far_groups = [list(range(len(UNITS[0]))), list(range(len(UNITS[0]), count - 2)), [count - 2], [count - 1]]

    def link(lane, u, owner, target):
        if lane == 2:
            recv = far_recv.at[next(g for g, group in enumerate(far_groups) if u in group)]
        else:
            recv = link_recv.at[u] if lane == u % 2 else rest_recv.at[units[u][0]]
        return copy(u, owner, link_send.at[units[u][0] // 2], recv, target)

    def across(lane, u, owner):
        return copy(u, owner, pair_send.at[units[u][0] // 2], pair_recv.at[units[u][0] // 2], pair)

    def sized(group):
        return og.at[pl.ds(0, sum(units[u][2] for u in group)), pl.ds(0, short)]

    def ahead(lane, k, src, target):
        cut = (whole, pl.ds(*pieces[k]))
        src = own.at[cut] if src is None else early.at[(src, *cut)]
        recv = early_recv.at[k if lane == k % 2 else EARLY]
        return remote(src, early.at[(lane, *cut)], early_send, recv, target)

    def send_own(u):
        link(0, u, me, near_x).start()
        link(1, u, me, near_y).start()
        across(3, u, me).start()

    compute(0)
    for key, f in fetches.items():
        if key not in urgent:
            f.start()
    pl.semaphore_wait(barrier, 3 + at.core * (model - 1))
    for u in range(1, count + 1):
        compute(u)
        send_own(u - 1)
    for u in range(count + 1, len(work)):
        compute(u)
    fetches["train"].wait()
    fetches["step"].wait()
    part[...] = jnp.zeros(part.shape, part.dtype)
    part[:, : nt.shape[1]] = nt[...] + ns[...]

    @pl.when(at.core == 1)
    def _():
        norm[chip, depth, 1] = part[...]

    def norm_copy(kind, ref, target):
        return remote(ref, ref, norm_send.at[kind], norm_recv.at[kind], target)

    def norm_part():
        return remote(part, norm.at[chip, depth, 0], norm_send.at[4], norm_recv.at[4], pair)

    def norm_whole():
        return norm_copy(3, norm, pair)

    def norm_step(u):
        if u == 1:
            norm_part().wait_recv()
            for step in range(1, model):
                norm_copy(0, norm.at[chip, depth], {"model": lax.rem(depth + step, model)}).start()
        if u == 2:
            came(norm.at[chip, pl.ds(0, model - 1)], norm_recv.at[0], near_x)
            norm_copy(1, norm.at[chip], near_x).start()
            norm_copy(1, norm.at[chip], near_y).start()
        if u == 3:
            came(norm.at[pl.ds(0, 2)], norm_recv.at[1], near_x)
            norm_copy(2, norm.at[near_x // 2], near_y).start()
        if u == 4:
            came(norm.at[chip], norm_recv.at[2], near_y)
            norm_whole().start()

    for u in range(count):
        a, lane = units[u][0], u % 2
        owner, target = ((near_x, near_y), (near_y, near_x))[lane]
        link(lane, u, owner, owner).wait_recv()
        link(2, u, owner, target).start()
        across(lane, u, owner).start()
        if u == count - 1 or units[u + 1][0] > a:
            group = [v for v in range(count) if units[v][0] == a]
            came(sized(group), rest_recv.at[a], near_x)
            for v in group:
                across(1 - v % 2, v, (near_y, near_x)[v % 2]).start()
        if u == 0:
            pl.when(at.core == 0)(lambda: norm_part().start())
        if 1 <= u <= 4:
            pl.when(at.core == 1)(functools.partial(norm_step, u))

    @pl.when(at.core == 1)
    def _():
        for k in range(EARLY):
            ahead(0, k, None, near_x).start()
            ahead(1, k, None, near_y).start()

    for g, group in enumerate(far_groups):
        came(sized(group), far_recv.at[g], near_x)
        for u in group:
            across(2, u, far).start()

    @pl.when(at.core == 1)
    def _():
        for k in range(EARLY):
            owner, target = ((near_x, near_y), (near_y, near_x))[k % 2]
            ahead(k % 2, k, None, owner).wait_recv()
            ahead(2, k, k % 2, target).start()

    @pl.when(at.core == 0)
    def _():
        norm_part().wait_send()
        norm_whole().wait_recv()

    @pl.when(at.core == 1)
    def _():
        sent(norm.at[chip, pl.ds(0, model - 1)], norm_send.at[0], near_x)
        sent(norm.at[pl.ds(0, 2)], norm_send.at[1], near_x)
        sent(norm.at[chip], norm_send.at[2], near_y)
        sent(norm, norm_send.at[3], pair)
        sent(early, early_send, near_x)
        came(early.at[pl.ds(0, 2)], early_recv.at[EARLY], near_x)

    sent(og.at[:, pl.ds(0, 2 * 3 * short)], link_send.at[0], near_x)
    sent(od.at[pl.ds(0, 3 * short_down)], link_send.at[1], near_x)
    sent(og, pair_send.at[0], pair)
    sent(od.at[pl.ds(0, 4 * short_down)], pair_send.at[1], pair)
    came(og, pair_recv.at[0], pair)
    came(od.at[pl.ds(0, 4 * short_down)], pair_recv.at[1], pair)


def second_kernel(own, early, token, down, link_send, link_recv, rest_recv, far_recv, pair_send, pair_recv, ready):
    at = Place()
    me, near_x, near_y, far, pair = at.me, at.near_x, at.near_y, at.far, at.pair
    short = own.shape[0]
    pieces = cuts(DOWN, own.shape[1])

    barrier = pltpu.get_barrier_semaphore()
    for other in (near_x, near_y):
        pl.semaphore_signal(barrier, inc=1, device_id={"rows": other}, device_id_type=MESH)
    pl.semaphore_wait(barrier, 2 + at.core)

    def cut(k):
        return slice(None), pl.ds(*pieces[k])

    def band(owner):
        return pl.ds(pl.multiple_of(owner * short, short), short)

    def place(k, owner):
        return down.at[band(owner), pl.ds(*pieces[k])]

    def link(lane, k, src, owner, target):
        recv = far_recv.at[k] if lane == 2 else link_recv.at[k] if lane == k % 2 else rest_recv
        return remote(src, place(k, owner), link_send, recv, target)

    def across(lane, k, src, owner):
        return remote(src, place(k, owner), pair_send, pair_recv, pair)

    def gather(first):
        late, everything = range(first, len(pieces)), range(len(pieces))
        for k in late:
            link(0, k, own.at[cut(k)], me, near_x).start()
            link(1, k, own.at[cut(k)], me, near_y).start()

        def over():
            for k in everything:
                across(3, k, own.at[cut(k)], me).start()
            for k in range(first):
                for lane, owner in enumerate((near_x, near_y, far)):
                    across(lane, k, early.at[(lane, *cut(k))], owner).start()

        if first:
            over()
        down[band(me), :] = own[...]
        if first:
            end = sum(pieces[first - 1])
            for lane, owner in enumerate((near_x, near_y, far)):
                down[band(owner), :end] = early[lane]
        width = own.shape[1] - pieces[first][0]
        for k in late:
            owner, target = ((near_x, near_y), (near_y, near_x))[k % 2]
            link(k % 2, k, place(k, owner), owner, owner).wait_recv()
            link(2, k, place(k, owner), owner, target).start()
        if not first:
            pl.semaphore_wait(ready, 1)
            over()
        came(down.at[pl.ds(0, short), pl.ds(0, width)], rest_recv, near_x)
        for k in late:
            across(0, k, place(k, near_x), near_x).start()
            across(1, k, place(k, near_y), near_y).start()
        for k in late:
            link(2, k, place(k, far), far, near_x).wait_recv()
            across(2, k, place(k, far), far).start()

        sent(down.at[pl.ds(0, 3 * short), pl.ds(0, width)], link_send, near_x)
        sent(down.at[pl.ds(0, 4 * short), :], pair_send, pair)
        came(down.at[pl.ds(0, 4 * short), :], pair_recv, pair)

    @pl.when(at.core == 0)
    def _():
        pl.semaphore_signal(barrier, inc=1, device_id={"rows": pair}, device_id_type=MESH)
        gather(0)

    @pl.when(at.core == 1)
    def _():
        pl.semaphore_signal(ready, inc=1, device_id={"rows": pair}, device_id_type=MESH)
        gather(EARLY)


HBM = pl.BlockSpec(memory_space=pltpu.HBM)
VMEM = pl.BlockSpec(memory_space=pltpu.VMEM)
MIB = 2**20
GRANT = 42


def first_gather(rows, model, arrays):
    weight_gate, weight_up, weight_down, norm_train = arrays[0], arrays[3], arrays[6], arrays[9]
    heads, pieces = down_cuts(weight_down.shape[0])
    short, head = weight_down.shape[1], sum(heads[-1])
    shapes = [
        (weight_gate.shape[1], weight_gate.shape[0] * rows),
        (weight_up.shape[1], weight_up.shape[0] * rows),
        (short * rows, head),
        (short, weight_down.shape[0] - head),
        (3, short, sum(pieces[EARLY - 1])),
    ]
    lanes = -(-norm_train.shape[1] // 128) * 128
    count = sum(len(parts) for parts in UNITS)
    dma = pltpu.SemaphoreType.DMA
    return pl.pallas_call(
        functools.partial(first_kernel, model),
        out_shape=[pltpu.VMEM(s, jnp.bfloat16) for s in shapes] + [pltpu.VMEM((rows // 2, model, 2, 1, lanes), jnp.float32)],
        in_specs=[HBM] * len(arrays),
        out_specs=[VMEM] * 6,
        scratch_shapes=[pltpu.VMEM(a.shape, a.dtype) for a in arrays]
        + [
            dma((13,)),
            dma((2,)), dma((count,)), dma((3,)), dma((4,)), dma((2,)), dma((2,)),
            dma(()), dma((EARLY + 1,)), dma((5,)), dma((5,)),
            pltpu.VMEM((1, lanes), jnp.float32),
        ],
        compiler_params=pltpu.CompilerParams(collective_id=0, has_side_effects=True, vmem_limit_bytes=GRANT * MIB),
    )(*arrays)


def second_gather(rows, own, early, token):
    dma = pltpu.SemaphoreType.DMA
    count = len(DOWN)
    return pl.pallas_call(
        second_kernel,
        out_shape=pltpu.VMEM((own.shape[0] * rows, own.shape[1]), jnp.bfloat16),
        in_specs=[VMEM, VMEM, HBM],
        out_specs=VMEM,
        scratch_shapes=[
            dma(()), dma((count,)), dma(()), dma((count,)), dma(()), dma(()), pltpu.SemaphoreType.REGULAR,
        ],
        compiler_params=pltpu.CompilerParams(collective_id=1, has_side_effects=True, vmem_limit_bytes=4 * MIB),
    )(own, early, token)


def write_kernel(size, g, u, d, norm, og, ou, od, out, token, packed_norm, sems):
    pairs = ((g, og), (u, ou), (d, od.at[:, pl.ds(0, d.shape[1])]), (packed_norm, out))
    copies = [pltpu.make_async_copy(s, t, sems.at[i]) for i, (s, t) in enumerate(pairs)]
    for c in copies[:3]:
        c.start()
    token[...] = jnp.zeros(token.shape, token.dtype)
    chips, model, cores, _, lanes = norm.shape
    parts = [norm[r, m, c][:, :size] for r in range(chips) for c in range(cores) for m in range(model)]
    group = lanes // size
    packed = [jnp.concatenate(parts[i : i + group], axis=1) for i in range(0, len(parts), group)]
    packed_norm[...] = jnp.concatenate(packed, axis=0).astype(out.dtype)
    copies[3].start()
    for c in copies:
        c.wait()


def written(size, gate, up, down, width, norm):
    chips, model, cores, _, lanes = norm.shape
    packed = (chips * model * cores * size // lanes, lanes)
    return pl.pallas_call(
        functools.partial(write_kernel, size),
        out_shape=[jax.ShapeDtypeStruct(s, jnp.bfloat16) for s in (gate.shape, up.shape, (down.shape[0], width), packed)]
        + [jax.ShapeDtypeStruct((8, 128), jnp.float32)],
        in_specs=[VMEM] * 4,
        out_specs=[HBM] * 4 + [VMEM],
        scratch_shapes=[pltpu.VMEM(packed, jnp.bfloat16), pltpu.SemaphoreType.DMA((4,))],
        compiler_params=pltpu.CompilerParams(vmem_limit_bytes=MIB),
    )(gate, up, down, norm)


def last_kernel(d, begun, od, sem):
    width = d.shape[1]
    c = pltpu.make_async_copy(d, od.at[:, pl.ds(od.shape[1] - width, width)], sem)
    c.start()
    c.wait()


def last_written(down, begun):
    return pl.pallas_call(
        last_kernel,
        out_shape=jax.ShapeDtypeStruct(begun.shape, begun.dtype),
        in_specs=[VMEM, HBM],
        out_specs=HBM,
        input_output_aliases={1: 0},
        scratch_shapes=[pltpu.SemaphoreType.DMA(())],
        compiler_params=pltpu.CompilerParams(vmem_limit_bytes=MIB),
    )(down, begun)


def local_kernel(rows, model, *arrays):
    arrays = tuple(a.T if i in (1, 4, 7) else a for i, a in enumerate(arrays[:9])) + tuple(
        a.reshape(1, -1) for a in arrays[9:]
    )
    gate, up, down, own, early, norm = first_gather(rows, model, arrays)
    gate, up, down, serve_norm, token = written(arrays[9].shape[1], gate, up, down, arrays[6].shape[0], norm)
    down = last_written(second_gather(rows, own, early, token), down)
    return gate, up, down, serve_norm.reshape(-1)


def merge(weight, low, high):
    full = weight.astype(jnp.float32) + mix_rate * jnp.dot(low, high, preferred_element_type=jnp.float32)
    return full.astype(jnp.bfloat16).T


def local_plain(*arrays):
    gate, up, down = merge(*arrays[:3]), merge(*arrays[3:6]), merge(*arrays[6:9])
    return (
        lax.all_gather(gate, "rows", axis=1, tiled=True),
        lax.all_gather(up, "rows", axis=1, tiled=True),
        lax.all_gather(down, "rows", axis=0, tiled=True),
        lax.all_gather((arrays[9] + arrays[10]).astype(jnp.bfloat16), ("rows", "model"), axis=0, tiled=True),
    )


def solution(mesh):
    rows, model = mesh.shape["rows"], mesh.shape["model"]
    local = functools.partial(local_kernel, rows, model) if rows == 2 * SIDE * SIDE else local_plain
    in_specs = (
        P("rows", "model"), P("rows", None), P(None, "model"),
        P("rows", "model"), P("rows", None), P(None, "model"),
        P("model", "rows"), P("model", None), P(None, "rows"),
        P(("rows", "model")), P(("rows", "model")),
    )
    out_specs = (P("model", None), P("model", None), P(None, "model"), P())
    return jax.shard_map(local, mesh=mesh, in_specs=in_specs, out_specs=out_specs, check_vma=False)
```

```python
import functools

import jax
import jax.numpy as jnp
from jax import lax
from jax.experimental import pallas as pl
from jax.experimental.pallas import tpu as pltpu
from jax.sharding import PartitionSpec as P

mix_rate = 0.5
MESH = pl.DeviceIdType.MESH
UNITS = ((2, 2, 2, 2, 4, 4), (4, 4, 4, 4), (1, 1))
DOWN = (4, 4, 2, 2, 1, 1)
EARLY = 4
SIDE = 2


def cuts(parts, size):
    whole = sum(parts)
    return [(sum(parts[:i]) * size // whole, parts[i] * size // whole) for i in range(len(parts))]


def down_cuts(size):
    pieces = cuts(UNITS[2] + DOWN, size)
    head = len(UNITS[2])
    offset = pieces[head][0]
    return pieces[:head], [(start - offset, length) for start, length in pieces[head:]]


class Place:
    def __init__(self):
        self.me = me = lax.axis_index("rows")
        self.core = core = lax.rem(me, 2)
        x = lax.rem(me // 2, SIDE)
        y = me // (2 * SIDE)

        def device(y, x, core):
            return (y * SIDE + x) * 2 + core

        self.near_x, self.near_y = device(y, 1 - x, core), device(1 - y, x, core)
        self.far = device(1 - y, 1 - x, core)
        self.pair = device(y, x, 1 - core)
        self.pair_x, self.pair_y = device(y, 1 - x, 1 - core), device(1 - y, x, 1 - core)
        self.pair_far = device(1 - y, 1 - x, 1 - core)


def remote(src, dst, send, recv, target):
    return pltpu.make_async_remote_copy(
        src_ref=src, dst_ref=dst, send_sem=send, recv_sem=recv,
        device_id=target if isinstance(target, dict) else {"rows": target}, device_id_type=MESH,
    )


def sent(ref, sem, other):
    remote(ref, ref, sem, sem, other).wait_send()


def came(ref, sem, other):
    remote(ref, ref, sem, sem, other).wait_recv()


def first_kernel(model, *refs):
    sources, (og, ou, od, own, early, norm), refs = refs[:11], refs[11:17], refs[17:]
    held, refs = refs[:11], refs[11:]
    wg, lg, hg, wu, lu, hu, wd, ld, hd, nt, ns = held
    fetch_sem, link_send, link_recv, rest_recv, far_recv, pair_send, pair_recv, early_send, early_recv, norm_send, norm_recv, part = refs
    at = Place()
    me, near_x, near_y, far, pair = at.me, at.near_x, at.near_y, at.far, at.pair
    depth = lax.axis_index("model")
    chip = me // 2

    outs = (og, ou, od)
    fetches = {}

    def fetch(key, i, *cut):
        fetches[key] = pltpu.make_async_copy(
            sources[i].at[cut] if cut else sources[i], held[i].at[cut] if cut else held[i],
            fetch_sem.at[len(fetches)],
        )

    short, short_down = wg.shape[0], wd.shape[1]
    heads, pieces = down_cuts(wd.shape[0])
    offset = sum(heads[-1])
    units = [(a, *cut) for a in range(2) for cut in cuts(UNITS[a], wg.shape[1])] + [(2, *cut) for cut in heads]
    count = len(units)
    work = units + [(2, offset + start, size) for start, size in pieces]
    whole = slice(None)

    first, rest = sum(units[1][1:]), wg.shape[1]
    fetch("low", 1)
    fetch("high", 2, whole, pl.ds(0, first))
    fetch("gate", 0, whole, pl.ds(0, first))
    fetch("high_rest", 2, whole, pl.ds(first, rest - first))
    fetch("gate_rest", 0, whole, pl.ds(first, rest - first))
    for a in (1, 2):
        for i in (1, 2, 0):
            fetch((a, i), 3 * a + i)
    fetch("train", 9)
    fetch("step", 10)
    urgent = ("low", "high", "gate")
    for key in urgent:
        fetches[key].start()

    barrier = pltpu.get_barrier_semaphore()
    for other in (near_x, near_y, pair):
        pl.semaphore_signal(barrier, inc=1, device_id={"rows": other}, device_id_type=MESH)

    @pl.when(at.core == 1)
    def _():
        for step in range(1, model):
            pl.semaphore_signal(barrier, inc=1, device_id={"model": lax.rem(depth + step, model)}, device_id_type=MESH)

    def place(u, owner):
        a, start, size = units[u]
        if a == 2:
            return od.at[pl.ds(pl.multiple_of(owner * short_down, short_down), short_down), pl.ds(start, size)]
        return outs[a].at[pl.ds(start, size), pl.ds(pl.multiple_of(owner * short, short), short)]

    def compute(u):
        a, start, size = work[u]
        if u == 0:
            needed = ("low", "high", "gate")
        elif u == 2:
            needed = ("high_rest", "gate_rest")
        elif a and work[u - 1][0] < a:
            needed = [(a, i) for i in range(3)]
        else:
            needed = ()
        for key in needed:
            fetches[key].wait()
        cut = slice(start, start + size)
        if a < 2:
            w, low, high = ((wg, lg, hg), (wu, lu, hu))[a]
            weight, low, high = w[:, cut], low[...], high[:, cut]
        else:
            weight, low, high = wd[cut, :], ld[:, cut], hd[...]
        merged = weight.astype(jnp.float32) + mix_rate * lax.dot_general(
            low, high, (((0,), (0,)), ((), ())), preferred_element_type=jnp.float32
        )
        merged = merged.astype(jnp.bfloat16).T
        if u < count:
            place(u, me)[...] = merged
        else:
            own[:, start - offset : start - offset + size] = merged

    def copy(u, owner, send, recv, target):
        return remote(place(u, owner), place(u, owner), send, recv, target)

    far_groups = [list(range(len(UNITS[0]))), list(range(len(UNITS[0]), count - 2)), [count - 2], [count - 1]]

    def link(lane, u, owner, target):
        if lane == 2:
            recv = far_recv.at[next(g for g, group in enumerate(far_groups) if u in group)]
        else:
            recv = link_recv.at[u] if lane == u % 2 else rest_recv.at[units[u][0]]
        return copy(u, owner, link_send.at[units[u][0] // 2], recv, target)

    def across(lane, u, owner):
        return copy(u, owner, pair_send.at[units[u][0] // 2], pair_recv.at[units[u][0] // 2], pair)

    def sized(group):
        return og.at[pl.ds(0, sum(units[u][2] for u in group)), pl.ds(0, short)]

    def ahead(lane, k, src, target):
        cut = (whole, pl.ds(*pieces[k]))
        src = own.at[cut] if src is None else early.at[(src, *cut)]
        recv = early_recv.at[k if lane == k % 2 else EARLY]
        return remote(src, early.at[(lane, *cut)], early_send, recv, target)

    def send_own(u):
        link(0, u, me, near_x).start()
        link(1, u, me, near_y).start()
        across(3, u, me).start()

    compute(0)
    for key, f in fetches.items():
        if key not in urgent:
            f.start()
    pl.semaphore_wait(barrier, 3 + at.core * (model - 1))
    for u in range(1, count + 1):
        compute(u)
        send_own(u - 1)
    for u in range(count + 1, len(work)):
        compute(u)
    fetches["train"].wait()
    fetches["step"].wait()
    part[...] = jnp.zeros(part.shape, part.dtype)
    part[:, : nt.shape[1]] = nt[...] + ns[...]

    @pl.when(at.core == 1)
    def _():
        norm[chip, depth, 1] = part[...]

    def norm_copy(kind, ref, target):
        return remote(ref, ref, norm_send.at[kind], norm_recv.at[kind], target)

    def norm_part():
        return remote(part, norm.at[chip, depth, 0], norm_send.at[4], norm_recv.at[4], pair)

    def norm_whole():
        return norm_copy(3, norm, pair)

    def norm_step(u):
        if u == 1:
            norm_part().wait_recv()
            for step in range(1, model):
                norm_copy(0, norm.at[chip, depth], {"model": lax.rem(depth + step, model)}).start()
        if u == 2:
            came(norm.at[chip, pl.ds(0, model - 1)], norm_recv.at[0], near_x)
            norm_copy(1, norm.at[chip], near_x).start()
            norm_copy(1, norm.at[chip], near_y).start()
        if u == 3:
            came(norm.at[pl.ds(0, 2)], norm_recv.at[1], near_x)
            norm_copy(2, norm.at[near_x // 2], near_y).start()
        if u == 4:
            came(norm.at[chip], norm_recv.at[2], near_y)
            norm_whole().start()

    for u in range(count):
        a, lane = units[u][0], u % 2
        owner, target = ((near_x, near_y), (near_y, near_x))[lane]
        link(lane, u, owner, owner).wait_recv()
        link(2, u, owner, target).start()
        across(lane, u, owner).start()
        if u == count - 1 or units[u + 1][0] > a:
            group = [v for v in range(count) if units[v][0] == a]
            came(sized(group), rest_recv.at[a], near_x)
            for v in group:
                across(1 - v % 2, v, (near_y, near_x)[v % 2]).start()
        if u == 0:
            pl.when(at.core == 0)(lambda: norm_part().start())
        if 1 <= u <= 4:
            pl.when(at.core == 1)(functools.partial(norm_step, u))

    @pl.when(at.core == 1)
    def _():
        for k in range(EARLY):
            ahead(0, k, None, near_x).start()
            ahead(1, k, None, near_y).start()

    for g, group in enumerate(far_groups):
        came(sized(group), far_recv.at[g], near_x)
        for u in group:
            across(2, u, far).start()

    @pl.when(at.core == 1)
    def _():
        for k in range(EARLY):
            owner, target = ((near_x, near_y), (near_y, near_x))[k % 2]
            ahead(k % 2, k, None, owner).wait_recv()
            ahead(2, k, k % 2, target).start()

    @pl.when(at.core == 0)
    def _():
        norm_part().wait_send()
        norm_whole().wait_recv()

    @pl.when(at.core == 1)
    def _():
        sent(norm.at[chip, pl.ds(0, model - 1)], norm_send.at[0], near_x)
        sent(norm.at[pl.ds(0, 2)], norm_send.at[1], near_x)
        sent(norm.at[chip], norm_send.at[2], near_y)
        sent(norm, norm_send.at[3], pair)
        sent(early, early_send, near_x)
        came(early.at[pl.ds(0, 2)], early_recv.at[EARLY], near_x)

    sent(og.at[:, pl.ds(0, 2 * 3 * short)], link_send.at[0], near_x)
    sent(od.at[pl.ds(0, 3 * short_down)], link_send.at[1], near_x)
    sent(og, pair_send.at[0], pair)
    sent(od.at[pl.ds(0, 4 * short_down)], pair_send.at[1], pair)
    came(og, pair_recv.at[0], pair)
    came(od.at[pl.ds(0, 4 * short_down)], pair_recv.at[1], pair)


def second_kernel(own, early, token, down, link_send, link_recv, rest_recv, far_recv, pair_send, pair_recv, ready):
    at = Place()
    me, near_x, near_y, far, pair = at.me, at.near_x, at.near_y, at.far, at.pair
    short = own.shape[0]
    pieces = cuts(DOWN, own.shape[1])

    barrier = pltpu.get_barrier_semaphore()
    for other in (near_x, near_y):
        pl.semaphore_signal(barrier, inc=1, device_id={"rows": other}, device_id_type=MESH)
    pl.semaphore_wait(barrier, 2 + at.core)

    def cut(k):
        return slice(None), pl.ds(*pieces[k])

    def band(owner):
        return pl.ds(pl.multiple_of(owner * short, short), short)

    def place(k, owner):
        return down.at[band(owner), pl.ds(*pieces[k])]

    def link(lane, k, src, owner, target):
        recv = far_recv.at[k] if lane == 2 else link_recv.at[k] if lane == k % 2 else rest_recv
        return remote(src, place(k, owner), link_send, recv, target)

    def across(lane, k, src, owner):
        return remote(src, place(k, owner), pair_send, pair_recv, pair)

    def gather(first):
        late, everything = range(first, len(pieces)), range(len(pieces))
        for k in late:
            link(0, k, own.at[cut(k)], me, near_x).start()
            link(1, k, own.at[cut(k)], me, near_y).start()

        def over():
            for k in everything:
                across(3, k, own.at[cut(k)], me).start()
            for k in range(first):
                for lane, owner in enumerate((near_x, near_y, far)):
                    across(lane, k, early.at[(lane, *cut(k))], owner).start()

        if first:
            over()
        if first:
            end = sum(pieces[first - 1])
            for lane, owner in enumerate((near_x, near_y, far)):
                down[band(owner), :end] = early[lane]
        width = own.shape[1] - pieces[first][0]
        for k in late:
            owner, target = ((near_x, near_y), (near_y, near_x))[k % 2]
            link(k % 2, k, place(k, owner), owner, owner).wait_recv()
            link(2, k, place(k, owner), owner, target).start()
        if not first:
            pl.semaphore_wait(ready, 1)
            over()
        came(down.at[pl.ds(0, short), pl.ds(0, width)], rest_recv, near_x)
        for k in late:
            across(0, k, place(k, near_x), near_x).start()
            across(1, k, place(k, near_y), near_y).start()
        for k in late:
            link(2, k, place(k, far), far, near_x).wait_recv()
            across(2, k, place(k, far), far).start()

        sent(down.at[pl.ds(0, 3 * short), pl.ds(0, width)], link_send, near_x)
        sent(down.at[pl.ds(0, 4 * short), :], pair_send, pair)
        came(down.at[pl.ds(0, 4 * short), :], pair_recv, pair)

    @pl.when(at.core == 0)
    def _():
        pl.semaphore_signal(barrier, inc=1, device_id={"rows": pair}, device_id_type=MESH)
        gather(0)

    @pl.when(at.core == 1)
    def _():
        pl.semaphore_signal(ready, inc=1, device_id={"rows": pair}, device_id_type=MESH)
        gather(EARLY)


HBM = pl.BlockSpec(memory_space=pltpu.HBM)
VMEM = pl.BlockSpec(memory_space=pltpu.VMEM)
MIB = 2**20
GRANT = 42


def first_gather(rows, model, arrays):
    weight_gate, weight_up, weight_down, norm_train = arrays[0], arrays[3], arrays[6], arrays[9]
    heads, pieces = down_cuts(weight_down.shape[0])
    short, head = weight_down.shape[1], sum(heads[-1])
    shapes = [
        (weight_gate.shape[1], weight_gate.shape[0] * rows),
        (weight_up.shape[1], weight_up.shape[0] * rows),
        (short * rows, head),
        (short, weight_down.shape[0] - head),
        (3, short, sum(pieces[EARLY - 1])),
    ]
    lanes = -(-norm_train.shape[1] // 128) * 128
    count = sum(len(parts) for parts in UNITS)
    dma = pltpu.SemaphoreType.DMA
    return pl.pallas_call(
        functools.partial(first_kernel, model),
        out_shape=[pltpu.VMEM(s, jnp.bfloat16) for s in shapes] + [pltpu.VMEM((rows // 2, model, 2, 1, lanes), jnp.float32)],
        in_specs=[HBM] * len(arrays),
        out_specs=[VMEM] * 6,
        scratch_shapes=[pltpu.VMEM(a.shape, a.dtype) for a in arrays]
        + [
            dma((13,)),
            dma((2,)), dma((count,)), dma((3,)), dma((4,)), dma((2,)), dma((2,)),
            dma(()), dma((EARLY + 1,)), dma((5,)), dma((5,)),
            pltpu.VMEM((1, lanes), jnp.float32),
        ],
        compiler_params=pltpu.CompilerParams(collective_id=0, has_side_effects=True, vmem_limit_bytes=GRANT * MIB),
    )(*arrays)


def second_gather(rows, own, early, token):
    dma = pltpu.SemaphoreType.DMA
    count = len(DOWN)
    return pl.pallas_call(
        second_kernel,
        out_shape=pltpu.VMEM((own.shape[0] * rows, own.shape[1]), jnp.bfloat16),
        in_specs=[VMEM, VMEM, HBM],
        out_specs=VMEM,
        scratch_shapes=[
            dma(()), dma((count,)), dma(()), dma((count,)), dma(()), dma(()), pltpu.SemaphoreType.REGULAR,
        ],
        compiler_params=pltpu.CompilerParams(collective_id=1, has_side_effects=True, vmem_limit_bytes=4 * MIB),
    )(own, early, token)


def write_kernel(size, g, u, d, own, norm, og, ou, od, out, token, packed_norm, sems):
    short = own.shape[0]
    mine = pl.ds(pl.multiple_of(lax.axis_index("rows") * short, short), short)
    pairs = (
        (g, og), (u, ou), (d, od.at[:, pl.ds(0, d.shape[1])]), (own, od.at[mine, pl.ds(d.shape[1], own.shape[1])]),
        (packed_norm, out),
    )
    copies = [pltpu.make_async_copy(s, t, sems.at[i]) for i, (s, t) in enumerate(pairs)]
    for c in copies[:4]:
        c.start()
    token[...] = jnp.zeros(token.shape, token.dtype)
    chips, model, cores, _, lanes = norm.shape
    parts = [norm[r, m, c][:, :size] for r in range(chips) for c in range(cores) for m in range(model)]
    group = lanes // size
    packed = [jnp.concatenate(parts[i : i + group], axis=1) for i in range(0, len(parts), group)]
    packed_norm[...] = jnp.concatenate(packed, axis=0).astype(out.dtype)
    copies[4].start()
    for c in copies:
        c.wait()


def written(size, gate, up, down, width, own, norm):
    chips, model, cores, _, lanes = norm.shape
    packed = (chips * model * cores * size // lanes, lanes)
    return pl.pallas_call(
        functools.partial(write_kernel, size),
        out_shape=[jax.ShapeDtypeStruct(s, jnp.bfloat16) for s in (gate.shape, up.shape, (down.shape[0], width), packed)]
        + [jax.ShapeDtypeStruct((8, 128), jnp.float32)],
        in_specs=[VMEM] * 5,
        out_specs=[HBM] * 4 + [VMEM],
        scratch_shapes=[pltpu.VMEM(packed, jnp.bfloat16), pltpu.SemaphoreType.DMA((5,))],
        compiler_params=pltpu.CompilerParams(vmem_limit_bytes=MIB),
    )(gate, up, down, own, norm)


def last_kernel(rows, d, begun, od, sems):
    me, width, short = lax.axis_index("rows"), d.shape[1], d.shape[0] // rows
    copies = []
    for step in range(1, rows):
        band = pl.ds(pl.multiple_of(lax.rem(me + step, rows) * short, short), short)
        copies.append(
            pltpu.make_async_copy(d.at[band], od.at[band, pl.ds(od.shape[1] - width, width)], sems.at[step - 1])
        )
    for c in copies:
        c.start()
    for c in copies:
        c.wait()


def last_written(rows, down, begun):
    return pl.pallas_call(
        functools.partial(last_kernel, rows),
        out_shape=jax.ShapeDtypeStruct(begun.shape, begun.dtype),
        in_specs=[VMEM, HBM],
        out_specs=HBM,
        input_output_aliases={1: 0},
        scratch_shapes=[pltpu.SemaphoreType.DMA((rows - 1,))],
        compiler_params=pltpu.CompilerParams(vmem_limit_bytes=MIB),
    )(down, begun)


def local_kernel(rows, model, *arrays):
    arrays = tuple(a.T if i in (1, 4, 7) else a for i, a in enumerate(arrays[:9])) + tuple(
        a.reshape(1, -1) for a in arrays[9:]
    )
    gate, up, down, own, early, norm = first_gather(rows, model, arrays)
    gate, up, down, serve_norm, token = written(arrays[9].shape[1], gate, up, down, arrays[6].shape[0], own, norm)
    down = last_written(rows, second_gather(rows, own, early, token), down)
    return gate, up, down, serve_norm.reshape(-1)


def merge(weight, low, high):
    full = weight.astype(jnp.float32) + mix_rate * jnp.dot(low, high, preferred_element_type=jnp.float32)
    return full.astype(jnp.bfloat16).T


def local_plain(*arrays):
    gate, up, down = merge(*arrays[:3]), merge(*arrays[3:6]), merge(*arrays[6:9])
    return (
        lax.all_gather(gate, "rows", axis=1, tiled=True),
        lax.all_gather(up, "rows", axis=1, tiled=True),
        lax.all_gather(down, "rows", axis=0, tiled=True),
        lax.all_gather((arrays[9] + arrays[10]).astype(jnp.bfloat16), ("rows", "model"), axis=0, tiled=True),
    )


def solution(mesh):
    rows, model = mesh.shape["rows"], mesh.shape["model"]
    local = functools.partial(local_kernel, rows, model) if rows == 2 * SIDE * SIDE else local_plain
    in_specs = (
        P("rows", "model"), P("rows", None), P(None, "model"),
        P("rows", "model"), P("rows", None), P(None, "model"),
        P("model", "rows"), P("model", None), P(None, "rows"),
        P(("rows", "model")), P(("rows", "model")),
    )
    out_specs = (P("model", None), P("model", None), P(None, "model"), P())
    return jax.shard_map(local, mesh=mesh, in_specs=in_specs, out_specs=out_specs, check_vma=False)
```

```python
import functools

import jax
import jax.numpy as jnp
from jax import lax
from jax.experimental import pallas as pl
from jax.experimental.pallas import tpu as pltpu
from jax.sharding import PartitionSpec as P

mix_rate = 0.5
MESH = pl.DeviceIdType.MESH
UNITS = ((1, 1, 6, 6, 1, 1), (7, 7, 1, 1), (1, 1))
DOWN = (4, 4, 2, 2, 1, 1)
EARLY = 4
SIDE = 2


def cuts(parts, size):
    whole = sum(parts)
    return [(sum(parts[:i]) * size // whole, parts[i] * size // whole) for i in range(len(parts))]


def down_cuts(size):
    pieces = cuts(UNITS[2] + DOWN, size)
    head = len(UNITS[2])
    offset = pieces[head][0]
    return pieces[:head], [(start - offset, length) for start, length in pieces[head:]]


class Place:
    def __init__(self):
        self.me = me = lax.axis_index("rows")
        self.core = core = lax.rem(me, 2)
        x = lax.rem(me // 2, SIDE)
        y = me // (2 * SIDE)

        def device(y, x, core):
            return (y * SIDE + x) * 2 + core

        self.near_x, self.near_y = device(y, 1 - x, core), device(1 - y, x, core)
        self.far = device(1 - y, 1 - x, core)
        self.pair = device(y, x, 1 - core)
        self.pair_x, self.pair_y = device(y, 1 - x, 1 - core), device(1 - y, x, 1 - core)
        self.pair_far = device(1 - y, 1 - x, 1 - core)


def remote(src, dst, send, recv, target):
    return pltpu.make_async_remote_copy(
        src_ref=src, dst_ref=dst, send_sem=send, recv_sem=recv,
        device_id=target if isinstance(target, dict) else {"rows": target}, device_id_type=MESH,
    )


def sent(ref, sem, other):
    remote(ref, ref, sem, sem, other).wait_send()


def came(ref, sem, other):
    remote(ref, ref, sem, sem, other).wait_recv()


def first_kernel(model, *refs):
    sources, (og, ou, od, own, early, norm), refs = refs[:11], refs[11:17], refs[17:]
    held, refs = refs[:11], refs[11:]
    wg, lg, hg, wu, lu, hu, wd, ld, hd, nt, ns = held
    fetch_sem, link_send, link_recv, rest_recv, far_recv, pair_send, pair_recv, early_send, early_recv, norm_send, norm_recv, part = refs
    at = Place()
    me, near_x, near_y, far, pair = at.me, at.near_x, at.near_y, at.far, at.pair
    depth = lax.axis_index("model")
    chip = me // 2

    outs = (og, ou, od)
    fetches = {}

    def fetch(key, i, *cut):
        fetches[key] = pltpu.make_async_copy(
            sources[i].at[cut] if cut else sources[i], held[i].at[cut] if cut else held[i],
            fetch_sem.at[len(fetches)],
        )

    short, short_down = wg.shape[0], wd.shape[1]
    heads, pieces = down_cuts(wd.shape[0])
    offset = sum(heads[-1])
    units = [(a, *cut) for a in range(2) for cut in cuts(UNITS[a], wg.shape[1])] + [(2, *cut) for cut in heads]
    count = len(units)
    work = units + [(2, offset + start, size) for start, size in pieces]
    whole = slice(None)

    first, rest = sum(units[1][1:]), wg.shape[1]
    fetch("low", 1)
    fetch("high", 2, whole, pl.ds(0, first))
    fetch("gate", 0, whole, pl.ds(0, first))
    fetch("high_rest", 2, whole, pl.ds(first, rest - first))
    fetch("gate_rest", 0, whole, pl.ds(first, rest - first))
    for a in (1, 2):
        for i in (1, 2, 0):
            fetch((a, i), 3 * a + i)
    fetch("train", 9)
    fetch("step", 10)
    urgent = ("low", "high", "gate")
    for key in urgent:
        fetches[key].start()

    barrier = pltpu.get_barrier_semaphore()
    for other in (near_x, near_y, pair):
        pl.semaphore_signal(barrier, inc=1, device_id={"rows": other}, device_id_type=MESH)

    @pl.when(at.core == 1)
    def _():
        for step in range(1, model):
            pl.semaphore_signal(barrier, inc=1, device_id={"model": lax.rem(depth + step, model)}, device_id_type=MESH)

    def place(u, owner):
        a, start, size = units[u]
        if a == 2:
            return od.at[pl.ds(pl.multiple_of(owner * short_down, short_down), short_down), pl.ds(start, size)]
        return outs[a].at[pl.ds(start, size), pl.ds(pl.multiple_of(owner * short, short), short)]

    def compute(u):
        a, start, size = work[u]
        if u == 0:
            needed = ("low", "high", "gate")
        elif u == 2:
            needed = ("high_rest", "gate_rest")
        elif a and work[u - 1][0] < a:
            needed = [(a, i) for i in range(3)]
        else:
            needed = ()
        for key in needed:
            fetches[key].wait()
        cut = slice(start, start + size)
        if a < 2:
            w, low, high = ((wg, lg, hg), (wu, lu, hu))[a]
            weight, low, high = w[:, cut], low[...], high[:, cut]
        else:
            weight, low, high = wd[cut, :], ld[:, cut], hd[...]
        merged = weight.astype(jnp.float32) + mix_rate * lax.dot_general(
            low, high, (((0,), (0,)), ((), ())), preferred_element_type=jnp.float32
        )
        merged = merged.astype(jnp.bfloat16).T
        if u < count:
            place(u, me)[...] = merged
        else:
            own[:, start - offset : start - offset + size] = merged

    def copy(u, owner, send, recv, target):
        return remote(place(u, owner), place(u, owner), send, recv, target)

    far_groups = [list(range(len(UNITS[0]))), list(range(len(UNITS[0]), count - 2)), [count - 2], [count - 1]]

    def link(lane, u, owner, target):
        if lane == 2:
            recv = far_recv.at[next(g for g, group in enumerate(far_groups) if u in group)]
        else:
            recv = link_recv.at[u] if lane == u % 2 else rest_recv.at[units[u][0]]
        return copy(u, owner, link_send.at[units[u][0] // 2], recv, target)

    def across(lane, u, owner):
        return copy(u, owner, pair_send.at[units[u][0] // 2], pair_recv.at[units[u][0] // 2], pair)

    def sized(group):
        return og.at[pl.ds(0, sum(units[u][2] for u in group)), pl.ds(0, short)]

    def ahead(lane, k, src, target):
        cut = (whole, pl.ds(*pieces[k]))
        src = own.at[cut] if src is None else early.at[(src, *cut)]
        recv = early_recv.at[k if lane == k % 2 else EARLY]
        return remote(src, early.at[(lane, *cut)], early_send, recv, target)

    def send_own(u):
        link(0, u, me, near_x).start()
        link(1, u, me, near_y).start()
        across(3, u, me).start()

    compute(0)
    for key, f in fetches.items():
        if key not in urgent:
            f.start()
    pl.semaphore_wait(barrier, 3 + at.core * (model - 1))
    for u in range(1, count + 1):
        compute(u)
        send_own(u - 1)
    for u in range(count + 1, len(work)):
        compute(u)
    fetches["train"].wait()
    fetches["step"].wait()
    part[...] = jnp.zeros(part.shape, part.dtype)
    part[:, : nt.shape[1]] = nt[...] + ns[...]

    @pl.when(at.core == 1)
    def _():
        norm[chip, depth, 1] = part[...]

    def norm_copy(kind, ref, target):
        return remote(ref, ref, norm_send.at[kind], norm_recv.at[kind], target)

    def norm_part():
        return remote(part, norm.at[chip, depth, 0], norm_send.at[4], norm_recv.at[4], pair)

    def norm_whole():
        return norm_copy(3, norm, pair)

    def norm_step(u):
        if u == 1:
            norm_part().wait_recv()
            for step in range(1, model):
                norm_copy(0, norm.at[chip, depth], {"model": lax.rem(depth + step, model)}).start()
        if u == 2:
            came(norm.at[chip, pl.ds(0, model - 1)], norm_recv.at[0], near_x)
            norm_copy(1, norm.at[chip], near_x).start()
            norm_copy(1, norm.at[chip], near_y).start()
        if u == 3:
            came(norm.at[pl.ds(0, 2)], norm_recv.at[1], near_x)
            norm_copy(2, norm.at[near_x // 2], near_y).start()
        if u == 4:
            came(norm.at[chip], norm_recv.at[2], near_y)
            norm_whole().start()

    for u in range(count):
        a, lane = units[u][0], u % 2
        owner, target = ((near_x, near_y), (near_y, near_x))[lane]
        link(lane, u, owner, owner).wait_recv()
        link(2, u, owner, target).start()
        across(lane, u, owner).start()
        if u == count - 1 or units[u + 1][0] > a:
            group = [v for v in range(count) if units[v][0] == a]
            came(sized(group), rest_recv.at[a], near_x)
            for v in group:
                across(1 - v % 2, v, (near_y, near_x)[v % 2]).start()
        if u == 0:
            pl.when(at.core == 0)(lambda: norm_part().start())
        if 1 <= u <= 4:
            pl.when(at.core == 1)(functools.partial(norm_step, u))

    @pl.when(at.core == 1)
    def _():
        for k in range(EARLY):
            ahead(0, k, None, near_x).start()
            ahead(1, k, None, near_y).start()

    for g, group in enumerate(far_groups):
        came(sized(group), far_recv.at[g], near_x)
        for u in group:
            across(2, u, far).start()

    @pl.when(at.core == 1)
    def _():
        for k in range(EARLY):
            owner, target = ((near_x, near_y), (near_y, near_x))[k % 2]
            ahead(k % 2, k, None, owner).wait_recv()
            ahead(2, k, k % 2, target).start()

    @pl.when(at.core == 0)
    def _():
        norm_part().wait_send()
        norm_whole().wait_recv()

    @pl.when(at.core == 1)
    def _():
        sent(norm.at[chip, pl.ds(0, model - 1)], norm_send.at[0], near_x)
        sent(norm.at[pl.ds(0, 2)], norm_send.at[1], near_x)
        sent(norm.at[chip], norm_send.at[2], near_y)
        sent(norm, norm_send.at[3], pair)
        sent(early, early_send, near_x)
        came(early.at[pl.ds(0, 2)], early_recv.at[EARLY], near_x)

    sent(og.at[:, pl.ds(0, 2 * 3 * short)], link_send.at[0], near_x)
    sent(od.at[pl.ds(0, 3 * short_down)], link_send.at[1], near_x)
    sent(og, pair_send.at[0], pair)
    sent(od.at[pl.ds(0, 4 * short_down)], pair_send.at[1], pair)
    came(og, pair_recv.at[0], pair)
    came(od.at[pl.ds(0, 4 * short_down)], pair_recv.at[1], pair)


def second_kernel(own, early, token, down, link_send, link_recv, rest_recv, far_recv, pair_send, pair_recv, ready):
    at = Place()
    me, near_x, near_y, far, pair = at.me, at.near_x, at.near_y, at.far, at.pair
    short = own.shape[0]
    pieces = cuts(DOWN, own.shape[1])

    barrier = pltpu.get_barrier_semaphore()
    for other in (near_x, near_y):
        pl.semaphore_signal(barrier, inc=1, device_id={"rows": other}, device_id_type=MESH)
    pl.semaphore_wait(barrier, 2 + at.core)

    def cut(k):
        return slice(None), pl.ds(*pieces[k])

    def band(owner):
        return pl.ds(pl.multiple_of(owner * short, short), short)

    def place(k, owner):
        return down.at[band(owner), pl.ds(*pieces[k])]

    def link(lane, k, src, owner, target):
        recv = far_recv.at[k] if lane == 2 else link_recv.at[k] if lane == k % 2 else rest_recv
        return remote(src, place(k, owner), link_send, recv, target)

    def across(lane, k, src, owner):
        return remote(src, place(k, owner), pair_send, pair_recv, pair)

    def gather(first):
        late, everything = range(first, len(pieces)), range(len(pieces))
        for k in late:
            link(0, k, own.at[cut(k)], me, near_x).start()
            link(1, k, own.at[cut(k)], me, near_y).start()

        def over():
            for k in everything:
                across(3, k, own.at[cut(k)], me).start()
            for k in range(first):
                for lane, owner in enumerate((near_x, near_y, far)):
                    across(lane, k, early.at[(lane, *cut(k))], owner).start()

        if first:
            over()
        if first:
            end = sum(pieces[first - 1])
            for lane, owner in enumerate((near_x, near_y, far)):
                down[band(owner), :end] = early[lane]
        width = own.shape[1] - pieces[first][0]
        for k in late:
            owner, target = ((near_x, near_y), (near_y, near_x))[k % 2]
            link(k % 2, k, place(k, owner), owner, owner).wait_recv()
            link(2, k, place(k, owner), owner, target).start()
        if not first:
            pl.semaphore_wait(ready, 1)
            over()
        came(down.at[pl.ds(0, short), pl.ds(0, width)], rest_recv, near_x)
        for k in late:
            across(0, k, place(k, near_x), near_x).start()
            across(1, k, place(k, near_y), near_y).start()
        for k in late:
            link(2, k, place(k, far), far, near_x).wait_recv()
            across(2, k, place(k, far), far).start()

        sent(down.at[pl.ds(0, 3 * short), pl.ds(0, width)], link_send, near_x)
        sent(down.at[pl.ds(0, 4 * short), :], pair_send, pair)
        came(down.at[pl.ds(0, 4 * short), :], pair_recv, pair)

    @pl.when(at.core == 0)
    def _():
        pl.semaphore_signal(barrier, inc=1, device_id={"rows": pair}, device_id_type=MESH)
        gather(0)

    @pl.when(at.core == 1)
    def _():
        pl.semaphore_signal(ready, inc=1, device_id={"rows": pair}, device_id_type=MESH)
        gather(EARLY)


HBM = pl.BlockSpec(memory_space=pltpu.HBM)
VMEM = pl.BlockSpec(memory_space=pltpu.VMEM)
MIB = 2**20
GRANT = 42


def first_gather(rows, model, arrays):
    weight_gate, weight_up, weight_down, norm_train = arrays[0], arrays[3], arrays[6], arrays[9]
    heads, pieces = down_cuts(weight_down.shape[0])
    short, head = weight_down.shape[1], sum(heads[-1])
    shapes = [
        (weight_gate.shape[1], weight_gate.shape[0] * rows),
        (weight_up.shape[1], weight_up.shape[0] * rows),
        (short * rows, head),
        (short, weight_down.shape[0] - head),
        (3, short, sum(pieces[EARLY - 1])),
    ]
    lanes = -(-norm_train.shape[1] // 128) * 128
    count = sum(len(parts) for parts in UNITS)
    dma = pltpu.SemaphoreType.DMA
    return pl.pallas_call(
        functools.partial(first_kernel, model),
        out_shape=[pltpu.VMEM(s, jnp.bfloat16) for s in shapes] + [pltpu.VMEM((rows // 2, model, 2, 1, lanes), jnp.float32)],
        in_specs=[HBM] * len(arrays),
        out_specs=[VMEM] * 6,
        scratch_shapes=[pltpu.VMEM(a.shape, a.dtype) for a in arrays]
        + [
            dma((13,)),
            dma((2,)), dma((count,)), dma((3,)), dma((4,)), dma((2,)), dma((2,)),
            dma(()), dma((EARLY + 1,)), dma((5,)), dma((5,)),
            pltpu.VMEM((1, lanes), jnp.float32),
        ],
        compiler_params=pltpu.CompilerParams(collective_id=0, has_side_effects=True, vmem_limit_bytes=GRANT * MIB),
    )(*arrays)


def second_gather(rows, own, early, token):
    dma = pltpu.SemaphoreType.DMA
    count = len(DOWN)
    return pl.pallas_call(
        second_kernel,
        out_shape=pltpu.VMEM((own.shape[0] * rows, own.shape[1]), jnp.bfloat16),
        in_specs=[VMEM, VMEM, HBM],
        out_specs=VMEM,
        scratch_shapes=[
            dma(()), dma((count,)), dma(()), dma((count,)), dma(()), dma(()), pltpu.SemaphoreType.REGULAR,
        ],
        compiler_params=pltpu.CompilerParams(collective_id=1, has_side_effects=True, vmem_limit_bytes=4 * MIB),
    )(own, early, token)


def write_kernel(size, g, u, d, own, norm, og, ou, od, out, token, packed_norm, sems):
    short = own.shape[0]
    mine = pl.ds(pl.multiple_of(lax.axis_index("rows") * short, short), short)
    pairs = (
        (g, og), (u, ou), (d, od.at[:, pl.ds(0, d.shape[1])]), (own, od.at[mine, pl.ds(d.shape[1], own.shape[1])]),
        (packed_norm, out),
    )
    copies = [pltpu.make_async_copy(s, t, sems.at[i]) for i, (s, t) in enumerate(pairs)]
    for c in copies[:4]:
        c.start()
    token[...] = jnp.zeros(token.shape, token.dtype)
    chips, model, cores, _, lanes = norm.shape
    parts = [norm[r, m, c][:, :size] for r in range(chips) for c in range(cores) for m in range(model)]
    group = lanes // size
    packed = [jnp.concatenate(parts[i : i + group], axis=1) for i in range(0, len(parts), group)]
    packed_norm[...] = jnp.concatenate(packed, axis=0).astype(out.dtype)
    copies[4].start()
    for c in copies:
        c.wait()


def written(size, gate, up, down, width, own, norm):
    chips, model, cores, _, lanes = norm.shape
    packed = (chips * model * cores * size // lanes, lanes)
    return pl.pallas_call(
        functools.partial(write_kernel, size),
        out_shape=[jax.ShapeDtypeStruct(s, jnp.bfloat16) for s in (gate.shape, up.shape, (down.shape[0], width), packed)]
        + [jax.ShapeDtypeStruct((8, 128), jnp.float32)],
        in_specs=[VMEM] * 5,
        out_specs=[HBM] * 4 + [VMEM],
        scratch_shapes=[pltpu.VMEM(packed, jnp.bfloat16), pltpu.SemaphoreType.DMA((5,))],
        compiler_params=pltpu.CompilerParams(vmem_limit_bytes=MIB),
    )(gate, up, down, own, norm)


def last_kernel(rows, d, begun, od, sems):
    me, width, short = lax.axis_index("rows"), d.shape[1], d.shape[0] // rows
    copies = []
    for step in range(1, rows):
        band = pl.ds(pl.multiple_of(lax.rem(me + step, rows) * short, short), short)
        copies.append(
            pltpu.make_async_copy(d.at[band], od.at[band, pl.ds(od.shape[1] - width, width)], sems.at[step - 1])
        )
    for c in copies:
        c.start()
    for c in copies:
        c.wait()


def last_written(rows, down, begun):
    return pl.pallas_call(
        functools.partial(last_kernel, rows),
        out_shape=jax.ShapeDtypeStruct(begun.shape, begun.dtype),
        in_specs=[VMEM, HBM],
        out_specs=HBM,
        input_output_aliases={1: 0},
        scratch_shapes=[pltpu.SemaphoreType.DMA((rows - 1,))],
        compiler_params=pltpu.CompilerParams(vmem_limit_bytes=MIB),
    )(down, begun)


def local_kernel(rows, model, *arrays):
    arrays = tuple(a.T if i in (1, 4, 7) else a for i, a in enumerate(arrays[:9])) + tuple(
        a.reshape(1, -1) for a in arrays[9:]
    )
    gate, up, down, own, early, norm = first_gather(rows, model, arrays)
    gate, up, down, serve_norm, token = written(arrays[9].shape[1], gate, up, down, arrays[6].shape[0], own, norm)
    down = last_written(rows, second_gather(rows, own, early, token), down)
    return gate, up, down, serve_norm.reshape(-1)


def merge(weight, low, high):
    full = weight.astype(jnp.float32) + mix_rate * jnp.dot(low, high, preferred_element_type=jnp.float32)
    return full.astype(jnp.bfloat16).T


def local_plain(*arrays):
    gate, up, down = merge(*arrays[:3]), merge(*arrays[3:6]), merge(*arrays[6:9])
    return (
        lax.all_gather(gate, "rows", axis=1, tiled=True),
        lax.all_gather(up, "rows", axis=1, tiled=True),
        lax.all_gather(down, "rows", axis=0, tiled=True),
        lax.all_gather((arrays[9] + arrays[10]).astype(jnp.bfloat16), ("rows", "model"), axis=0, tiled=True),
    )


def solution(mesh):
    rows, model = mesh.shape["rows"], mesh.shape["model"]
    local = functools.partial(local_kernel, rows, model) if rows == 2 * SIDE * SIDE else local_plain
    in_specs = (
        P("rows", "model"), P("rows", None), P(None, "model"),
        P("rows", "model"), P("rows", None), P(None, "model"),
        P("model", "rows"), P("model", None), P(None, "rows"),
        P(("rows", "model")), P(("rows", "model")),
    )
    out_specs = (P("model", None), P("model", None), P(None, "model"), P())
    return jax.shard_map(local, mesh=mesh, in_specs=in_specs, out_specs=out_specs, check_vma=False)
```
